32 devices in a mesh: sub: 16 (over z, x, core), chan: 2 (over y).
Axes of the slice: x: 2, y: 2, z: 4, core: 2. Of those that a mesh axis runs over, the one named last changes fastest.
Arguments:
- raw_pulses: bfloat16 [2, 512, 2, 2048], P(None, 'sub', 'chan'), may hold values from -6 to 6
- range_filter: bfloat16 [2, 2048, 1024], P(None, ('sub', 'chan')), may hold values from -0.09375 to 0.09375
- channel_mix: float32 [2, 32, 2, 2], replicated, may hold values from -3 to 3
- steer_angles: float32 [256], replicated, may hold values from -3.140625 to 3.140625
- band_offsets: int32 [4, 512], replicated, may hold values from 0 to 248
- band_weights: float32 [4, 2, 2, 512, 8], replicated, may hold values from -1 to 1
- smoothing: float32 [4096], P('sub'), may hold values from 0.3 to 0.5
Outputs:
- despeckled: float32 [4096, 1024], P('sub', 'chan')
The draws below stay inside these ranges and needn't reach their ends.
All inputs are finite; a program needn't handle non-finite values.
Results may differ from the reference program's by a relative error of at most 0.0036.
Values may be sent and summed in bfloat16 or wider, within the bound.
A program may use at most 64 MiB of HBM per device.

```python
import jax
import jax.numpy as jnp
import numpy as np
from jax import lax

P_DEV = 32
SAMPLES = 2048
BINS = 1024
ANG = 256
BAND = 8
LEVELS = 4
PASSES = 3
CHANNELS = 2
PULSES = 512
ANGLES = 4096
N_SUB = 16


def set_ends(entries, key, least, top_value):
    index_at = [jax.random.randint(jax.random.fold_in(key, axis), (), 0, length) for axis, length in enumerate(entries.shape)]
    main_axis = entries.shape.index(max(entries.shape))
    next_to = index_at[:main_axis] + [(index_at[main_axis] + 1) % entries.shape[main_axis]] + index_at[main_axis + 1:]
    return entries.at[tuple(index_at)].set(least).at[tuple(next_to)].set(top_value)


def level_of(own_key, extent, split, least, top_value):
    factor_of = 1.0
    for dim, parts in split:
        steps = jax.random.uniform(jax.random.fold_in(jax.random.fold_in(own_key, 6), dim), (parts,), jnp.float32, least / len(split), top_value / len(split))
        factor_of = factor_of * jnp.repeat(jnp.exp(steps), extent[dim] // parts).reshape((-1,) + (1,) * (len(extent) - 1 - dim))
    return factor_of


def scatter_about(own_key, extent, deviation, most, split=(), kind=jnp.bfloat16):
    loudness = level_of(own_key, extent, split, -0.22, 0.18) if split else 1.0
    values = jax.random.normal(own_key, extent, jnp.float32) * deviation * loudness
    return jnp.minimum(jnp.maximum(values, -most), most).astype(kind)


def setup_inputs(seed: int = 0) -> dict:
    keys = jax.random.split(jax.random.key(seed), 8)
    return {
        "raw_pulses": scatter_about(keys[0], (2, PULSES, CHANNELS, SAMPLES), 1.0, 6.0, ((1, 16), (2, 2))),
        "range_filter": scatter_about(keys[1], (2, SAMPLES, BINS), (2 * SAMPLES) ** -0.5, 0.09375, ((1, 32),)),
        "channel_mix": scatter_about(keys[2], (2, P_DEV, CHANNELS, CHANNELS), (2 * CHANNELS) ** -0.5, 3.0, (), jnp.float32),
        "steer_angles": jnp.clip(jax.random.uniform(keys[3], (ANG,), jnp.float32, -3.140625, 3.140625), -3.140625, 3.140625),
        "band_offsets": set_ends(jax.random.randint(keys[4], (LEVELS, 2 * ANG), 0, ANG - BAND + 1), jax.random.fold_in(keys[4], 1), 0, ANG - BAND).astype(jnp.int32),
        "band_weights": scatter_about(keys[5], (LEVELS, 2, 2, 2 * ANG, BAND), (4 * BAND) ** -0.5, 1.0, (), jnp.float32),
        "smoothing": jnp.clip(0.3 + 0.19999999 * jax.random.uniform(keys[6], (ANGLES,), jnp.float32) ** level_of(keys[6], (ANGLES,), ((0, 16),), -0.2, 0.2), 0.3, 0.5),
    }


HIGH = lax.Precision.HIGHEST

def doppler_table(count):
    index_row = jnp.arange(count, dtype=jnp.int32)
    product = index_row[:, None] * index_row[None, :] % count
    phase = 2.0 * np.pi / count * product.astype(jnp.float32)
    factor = 1.0 / np.sqrt(count)
    return ((jnp.cos(phase) * factor).astype(jnp.bfloat16), (-jnp.sin(phase) * factor).astype(jnp.bfloat16))

def steer_table(steer_angles, count):
    offsets = jnp.arange(count, dtype=jnp.int32).astype(jnp.float32) - 0.5 * count
    phase = steer_angles[:, None] * offsets[None, :]
    factor = 1.0 / np.sqrt(count)
    return ((jnp.cos(phase) * factor).astype(jnp.bfloat16), (jnp.sin(phase) * factor).astype(jnp.bfloat16))

def low_dot(left, right):
    return jnp.dot(left, right, preferred_element_type=jnp.float32)

def range_terms(echo_rows, filter_rows):
    real_part = low_dot(echo_rows[0], filter_rows[0]) - low_dot(echo_rows[1], filter_rows[1])
    imag_part = low_dot(echo_rows[0], filter_rows[1]) + low_dot(echo_rows[1], filter_rows[0])
    return jnp.stack([real_part, imag_part])

def form_image(compressed, dop_real, dop_imag, channel_mix, beam_real, beam_imag):
    pulse_count = compressed.shape[1]
    channels = compressed.shape[2]
    cells = compressed.shape[3]
    flat = compressed.reshape(2, pulse_count, channels * cells)
    spec_real = (low_dot(dop_real, flat[0]) - low_dot(dop_imag, flat[1])).reshape(pulse_count, channels, cells)
    spec_imag = (low_dot(dop_real, flat[1]) + low_dot(dop_imag, flat[0])).reshape(pulse_count, channels, cells)
    mix_real = jnp.einsum('fkc,fcb->kfb', channel_mix[0], spec_real, precision=HIGH) - jnp.einsum('fkc,fcb->kfb', channel_mix[1], spec_imag, precision=HIGH)
    mix_imag = jnp.einsum('fkc,fcb->kfb', channel_mix[0], spec_imag, precision=HIGH) + jnp.einsum('fkc,fcb->kfb', channel_mix[1], spec_real, precision=HIGH)
    recon = jnp.stack([mix_real, mix_imag]).astype(jnp.bfloat16).reshape(2, channels * pulse_count, cells)
    image_real = low_dot(beam_real, recon[0]) - low_dot(beam_imag, recon[1])
    image_imag = low_dot(beam_real, recon[1]) + low_dot(beam_imag, recon[0])
    return jnp.stack([image_real, image_imag])

def band_matrix(offsets, weights, count):
    band_width = weights.shape[-1]
    columns = jnp.arange(count, dtype=jnp.int32)
    stepping = jnp.arange(band_width, dtype=jnp.int32)
    target = offsets.astype(jnp.int32)[:, None, None] + stepping[None, :, None]
    hitting = (columns[None, None, :] == target).astype(jnp.float32)
    return jnp.einsum('crkj,kja->crka', weights, hitting, precision=HIGH)

def batched_apply(matrices, field):
    real_part = jnp.einsum('dka,dab->dkb', matrices[0], field[:, 0], precision=HIGH) - jnp.einsum('dka,dab->dkb', matrices[1], field[:, 1], precision=HIGH)
    imag_part = jnp.einsum('dka,dab->dkb', matrices[0], field[:, 1], precision=HIGH) + jnp.einsum('dka,dab->dkb', matrices[1], field[:, 0], precision=HIGH)
    return jnp.stack([real_part, imag_part], axis=1)

def reference(raw_pulses, range_filter, channel_mix, steer_angles, band_offsets, band_weights, smoothing):
    channels = raw_pulses.shape[2]
    blocks = jnp.moveaxis(raw_pulses.reshape(2, N_SUB, P_DEV, channels, SAMPLES), 1, 0)
    dop_real, dop_imag = doppler_table(P_DEV)
    beam_real, beam_imag = steer_table(steer_angles, channels * P_DEV)

    def one_block(block):
        echo_rows = block.reshape(2, P_DEV * channels, SAMPLES)
        compressed = range_terms(echo_rows, range_filter).astype(jnp.bfloat16).reshape(2, P_DEV, channels, BINS)
        return form_image(compressed, dop_real, dop_imag, channel_mix, beam_real, beam_imag)
    images = lax.map(one_block, blocks)
    index_all = np.arange(N_SUB)
    for merge_level in range(LEVELS):
        bit_value = 1 << merge_level
        lower_index = index_all & ~bit_value
        upper_index = index_all | bit_value
        half_index = index_all >> merge_level & 1
        full_band = band_matrix(band_offsets[merge_level], band_weights[merge_level], ANG)
        full_band = full_band.reshape(2, 2, 2, ANG, ANG)
        chosen = full_band[:, :, half_index]
        images = batched_apply(chosen[0], images[lower_index]) + batched_apply(chosen[1], images[upper_index])
    power = images[:, 0] * images[:, 0] + images[:, 1] * images[:, 1]
    power = power.reshape(N_SUB * ANG, BINS)
    rate = smoothing[:, None]
    for sweep in range(PASSES):
        padded = jnp.pad(power, ((0, 0), (1, 1)))
        power = power + rate * (padded[:, :-2] - 2.0 * power + padded[:, 2:])
    return power
```

```python
import functools

import jax
import jax.numpy as jnp
import numpy as np
from jax import lax
from jax.experimental import pallas as pl
from jax.experimental.pallas import tpu as pltpu
from jax.sharding import PartitionSpec as P

PASSES = 3
HALO = 16
LANES = 128
HIGH = lax.Precision.HIGHEST
LOW = jnp.bfloat16
MESH = pl.DeviceIdType.MESH
def rounded(value):
    return lax.reduce_precision(value, exponent_bits=8, mantissa_bits=7)


def halves(value):
    top = rounded(value)
    return top.astype(LOW), (value - top).astype(LOW)


def doppler_table(count):
    index_row = jnp.arange(count, dtype=jnp.int32)
    product = index_row[:, None] * index_row[None, :] % count
    phase = 2.0 * np.pi / count * product.astype(jnp.float32)
    factor = 1.0 / np.sqrt(count)
    return (
        rounded(jnp.cos(phase) * factor),
        rounded(-jnp.sin(phase) * factor),
    )


def steer_table(steer_angles, count):
    offsets = jnp.arange(count, dtype=jnp.int32).astype(jnp.float32) - 0.5 * count
    phase = offsets[:, None] * steer_angles[None, :]
    factor = 1.0 / np.sqrt(count)
    return (
        rounded(jnp.cos(phase) * factor),
        rounded(jnp.sin(phase) * factor),
    )


def forming_operator(channel_mix, steer_angles, pulse_count):
    channels = channel_mix.shape[2]
    dop_r, dop_i = doppler_table(pulse_count)
    beam_r, beam_i = steer_table(steer_angles, channels * pulse_count)
    mix = channel_mix.transpose(0, 3, 2, 1)[:, :, None, :, :]
    dr, di = dop_r.T[None, :, None, :], dop_i.T[None, :, None, :]
    shape = (channels * pulse_count, channels * pulse_count)
    mixed_r = (mix[0] * dr - mix[1] * di).reshape(shape)
    mixed_i = (mix[0] * di + mix[1] * dr).reshape(shape)
    left = jnp.concatenate([mixed_r, mixed_i], axis=1)
    t_r = jnp.dot(left, jnp.concatenate([beam_r, -beam_i], axis=0), precision=HIGH)
    t_i = jnp.dot(left, jnp.concatenate([beam_i, beam_r], axis=0), precision=HIGH)
    angles = steer_angles.shape[0]
    t_r = t_r.reshape(channels, pulse_count, angles)
    t_i = t_i.reshape(channels, pulse_count, angles)
    top = jnp.concatenate([t_r, t_i], axis=2)
    low = jnp.concatenate([-t_i, t_r], axis=2)
    both = jnp.concatenate([top, low], axis=1)
    return both.reshape(channels * 2 * pulse_count, 2 * angles)


def operator_body(offsets_ref, weights_ref, *out_refs):
    band_width, count = weights_ref.shape[3], weights_ref.shape[4]
    delta = lax.broadcasted_iota(jnp.int32, (count, count), 0) - offsets_ref[0]
    bands = [jnp.zeros((count, count), jnp.float32)] * 2
    for j in range(band_width):
        hit = delta == j
        bands = [
            jnp.where(hit, weights_ref[0, 0, part, j : j + 1, :], bands[part]) for part in range(2)
        ]
    for order, ref in enumerate(out_refs):
        real, imag = (band.astype(LOW) for band in bands)
        ref[0, 0, :count, :count] = real
        ref[0, 0, :count, count:] = imag
        ref[0, 0, count:, :count] = -imag
        ref[0, 0, count:, count:] = real
        if order + 1 < len(out_refs):
            bands = [band - band.astype(LOW).astype(jnp.float32) for band in bands]


def merge_operators(offsets, weights, parts):
    levels, _, _, merged, band_width = weights.shape
    count = merged // 2
    by_step = weights.transpose(0, 1, 2, 4, 3)
    shape = jax.ShapeDtypeStruct((levels, 2, 2 * count, 2 * merged), LOW)
    return pl.pallas_call(
        operator_body,
        grid=(levels, 2, 2),
        in_specs=[
            pl.BlockSpec((1, 1, count), lambda l, c, h: (l, 0, h)),
            pl.BlockSpec((1, 1, 2, band_width, count), lambda l, c, h: (l, c, 0, 0, h)),
        ],
        out_specs=[
            pl.BlockSpec((1, 1, 2 * count, 2 * count), lambda l, c, h: (l, c, 0, h))
        ] * parts,
        out_shape=[shape] * parts,
        cost_estimate=pl.CostEstimate(
            flops=levels * 4 * count * count * 32,
            bytes_accessed=levels * parts * 16 * count * count * 2,
            transcendentals=0,
        ),
    )(offsets[:, None, :], by_step)


def low_dot(left, right):
    return jnp.dot(left, right, preferred_element_type=jnp.float32)


def local_plain(
    raw_pulses, range_filter, channel_mix, steer_angles, band_offsets, band_weights, smoothing
):
    pulses = raw_pulses.shape[1]
    samples = raw_pulses.shape[3]
    bins = range_filter.shape[2]
    angles = steer_angles.shape[0]
    levels = band_offsets.shape[0]
    subs, chans = lax.axis_size("sub"), lax.axis_size("chan")
    own = bins // (subs * chans)

    part = lax.all_to_all(range_filter, "chan", split_axis=2, concat_axis=1, tiled=True)
    filt = lax.all_gather(part, "sub", axis=1, tiled=True)
    echo = lax.all_gather(raw_pulses[:, :, 0, :], "chan", axis=0)

    forming = forming_operator(channel_mix, steer_angles, pulses)
    form_top, form_low = halves(forming)
    base_top, base_low = merge_operators(band_offsets[:1], band_weights[:1], 2)
    folded = [
        low_dot(form_top, base_top[0, c])
        + (low_dot(form_low, base_top[0, c]) + low_dot(form_top, base_low[0, c]))
        for c in range(2)
    ]
    folded_top, folded_low = halves(jnp.concatenate(folded, axis=0))
    (later,) = merge_operators(band_offsets[1:], band_weights[1:], 1)

    real_rows = jnp.concatenate([echo[:, 0], -echo[:, 1]], axis=2)
    imag_rows = jnp.concatenate([echo[:, 1], echo[:, 0]], axis=2)
    stacked = jnp.concatenate([real_rows, imag_rows], axis=1).reshape(-1, 2 * samples)
    compressed = low_dot(stacked, filt.reshape(2 * samples, -1)).astype(LOW)
    blocks = compressed.T.reshape(subs, own, -1)
    got = lax.all_to_all(blocks, "sub", split_axis=0, concat_axis=0, tiled=True)
    image = got.reshape(subs * own, -1)
    for level in range(levels):
        run = (1 << level) * own
        wide = image.shape[1]
        field = image.astype(LOW).reshape(-1, 2, run, wide)
        pair = jnp.concatenate([field[:, 0], field[:, 1]], axis=2).reshape(-1, 2 * wide)
        if level == 0:
            out = low_dot(pair, folded_top) + low_dot(pair, folded_low)
        else:
            out = low_dot(pair, later[level - 1].reshape(2 * wide, -1))
        out = out.reshape(-1, run, 4 * angles)
        image = jnp.stack([out[:, :, : 2 * angles], out[:, :, 2 * angles :]], axis=1)
        image = image.reshape(-1, 2 * angles)
    power = image[:, :angles] * image[:, :angles] + image[:, angles:] * image[:, angles:]
    power = power.astype(LOW).reshape(subs, own, angles)
    power = lax.all_to_all(power, "sub", split_axis=0, concat_axis=0, tiled=True)
    power = power.reshape(subs * own, angles)
    up = [(i, i + 1) for i in range(chans - 1)]
    down = [(j, i) for i, j in up]
    before = lax.ppermute(power[-PASSES:], "chan", up).astype(jnp.float32)
    after = lax.ppermute(power[:PASSES], "chan", down).astype(jnp.float32)
    power = jnp.concatenate([before, power.astype(jnp.float32), after], axis=0)
    rate = smoothing[None, :]
    at = lax.axis_index("chan")
    lead, trail = at == 0, at == chans - 1
    for sweep in range(PASSES):
        mid = power[1:-1]
        power = mid + rate * (power[:-2] - 2.0 * mid + power[2:])
        edge = PASSES - 1 - sweep
        if edge:
            inner = power[edge:-edge]
            head = jnp.where(lead, 0.0, power[:edge])
            tail = jnp.where(trail, 0.0, power[-edge:])
            power = jnp.concatenate([head, inner, tail], axis=0)
    return power.T


def flip(value, bits):
    out = value
    step = 1
    while step <= bits:
        if bits & step:
            out = out + step - 2 * step * ((value // step) % 2)
        step *= 2
    return out


def forming_rows(channel_mix, steer_angles, pulse_count):
    channels = channel_mix.shape[2]
    dop_r, dop_i = doppler_table(pulse_count)
    beam_r, beam_i = steer_table(steer_angles, channels * pulse_count)
    mix = channel_mix.transpose(0, 3, 2, 1)[:, :, None, :, :]
    dr, di = dop_r.T[None, :, None, :], dop_i.T[None, :, None, :]
    shape = (channels * pulse_count, channels * pulse_count)
    mixed_r = (mix[0] * dr - mix[1] * di).reshape(shape)
    mixed_i = (mix[0] * di + mix[1] * dr).reshape(shape)
    left = jnp.concatenate([mixed_r, mixed_i], axis=1)
    t_r = jnp.dot(left, jnp.concatenate([beam_r, -beam_i], axis=0), precision=HIGH)
    t_i = jnp.dot(left, jnp.concatenate([beam_i, beam_r], axis=0), precision=HIGH)
    top = jnp.concatenate([t_r, t_i], axis=1)
    low = jnp.concatenate([-t_i, t_r], axis=1)
    return jnp.concatenate([top, low], axis=0)


def window_body(
    subs,
    filt_hbm,
    raw_hbm,
    form_ref,
    offs_ref,
    wts_ref,
    out_ref,
    bsrc,
    ys,
    bg,
    echo,
    acc,
    base_hi,
    base_lo,
    fold_hi,
    fold_lo,
    ops,
    sbuf,
    img0,
    img_a,
    img_b,
    pbuf,
    rows_c,
    loc_sem,
    y_s,
    y_r,
    bz_s,
    bz_r,
    bx_s,
    bx_r,
    a_s,
    a_r,
    sb_s,
    sb_r,
    sc_s,
    sc_r,
    h_s,
    h_r,
):
    chans = 2
    rows = bsrc.shape[1]
    half = ys.shape[2]
    pulses = echo.shape[3]
    own = img0.shape[2]
    angles = form_ref.shape[1] // 2
    depth = subs // 4
    group = subs // 4
    levels = offs_ref.shape[0]

    s, c = lax.axis_index("sub"), lax.axis_index("chan")
    z, x, k = s // 4, (s // 2) % 2, s % 2
    par, zp = z % 2, z // 2

    def sub_at(dz, dx, dk):
        return flip(z, dz) * 4 + flip(x, dx) * 2 + flip(k, dk)

    def device(dz, dx, dk, dc):
        return {"sub": sub_at(dz, dx, dk), "chan": flip(c, dc)}

    def remote(src, dst, send, recv, dev):
        return pltpu.make_async_remote_copy(
            src_ref=src, dst_ref=dst, send_sem=send, recv_sem=recv, device_id=dev, device_id_type=MESH
        )

    q_me = par * 2 + k
    load_b = pltpu.make_async_copy(filt_hbm, bsrc, loc_sem.at[0])
    load_a = pltpu.make_async_copy(raw_hbm, echo.at[q_me, :, c], loc_sem.at[1])
    load_b.start()
    load_a.start()

    barrier = pltpu.get_barrier_semaphore()
    greeted = [(0, 0, 0, 1), (0, 1, 0, 0)]
    greeted += [(dz, 0, dk, 0) for dz in range(depth) for dk in range(2) if dz or dk]
    for who in greeted:
        pl.semaphore_signal(barrier, inc=1, device_id=device(*who), device_id_type=MESH)
    pl.semaphore_wait(barrier, len(greeted))

    sent = []

    def go(copy):
        copy.start()
        sent.append(copy)

    def spot(dz, dx, dk, dc):
        at = (sub_at(dz, dx, dk) * chans + flip(c, dc)) * rows
        return bg.at[:, pl.ds(pl.multiple_of(at, rows), rows), :]

    def column(dz, dk):
        return ((flip(z, dz) % 2) * 2 + flip(k, dk)) * LANES

    def piece(dz, dk, dc):
        if dc:
            return ys.at[:, :, pl.ds(pl.multiple_of(column(dz, dk), LANES), LANES)]
        at = c * half + column(dz, dk)
        return bsrc.at[:, :, pl.ds(pl.multiple_of(at, LANES), LANES)]

    def block(dz, dk, dc):
        return remote(
            piece(dz, dk, dc), spot(0, 0, 0, dc), bz_s.at[dz, dk, dc], bz_r.at[dz, dk, dc], device(dz, 0, dk, 0)
        )

    def arrived(dz, dk, dc):
        remote(
            piece(dz, dk, dc), spot(dz, 0, dk, dc), bz_s.at[dz, dk, dc], bz_r.at[dz, dk, dc], device(dz, 0, dk, 0)
        ).wait_recv()

    def across(dz, dk, dc):
        return remote(
            spot(dz, 0, dk, dc), spot(dz, 0, dk, dc), bx_s.at[dz, dk, dc], bx_r.at[dz, dk, dc], device(0, 1, 0, 0)
        )

    def crossed(dz, dk, dc):
        remote(
            spot(dz, 1, dk, dc), spot(dz, 1, dk, dc), bx_s.at[dz, dk, dc], bx_r.at[dz, dk, dc], device(0, 1, 0, 0)
        ).wait_recv()

    def echo_at(da, dk, dc):
        return echo.at[flip(par, da) * 2 + flip(k, dk), :, flip(c, dc)]

    def pass_echo(slot, here, there, dev):
        spot_here = echo_at(*here)
        go(remote(spot_here, spot_here, a_s.at[slot], a_r.at[there[0], there[1], there[2]], device(*dev)))

    def echo_in(da, dk, dc):
        there = echo_at(da, dk, dc)
        remote(there, there, a_s.at[0], a_r.at[da, dk, dc], device(0, 0, 0, 1)).wait_recv()

    def build(level, side):
        block_rows = 32
        lane = side * angles
        offs = offs_ref[level, :, lane : lane + angles]

        def strip(i, carry):
            at = pl.multiple_of(i * block_rows, block_rows)
            delta = lax.broadcasted_iota(jnp.int32, (block_rows, angles), 0) + at - offs
            band = [[jnp.zeros((block_rows, angles), jnp.float32)] * 2 for _ in range(2)]
            for j in range(wts_ref.shape[3]):
                hit = delta == j
                for child in range(2):
                    for part in range(2):
                        row = wts_ref[level, child, part, j : j + 1, lane : lane + angles]
                        band[child][part] = jnp.where(hit, row, band[child][part])
            left = 2 * lane
            for child in range(2):
                real, imag = band[child]
                for order in range(2 if level == 0 else 1):
                    r, m = real.astype(LOW), imag.astype(LOW)
                    if level == 0:
                        ref = (base_hi if order == 0 else base_lo).at[child]
                    else:
                        ref = ops.at[level - 1, child]
                    low = pl.ds(pl.multiple_of(angles + at, block_rows), block_rows)
                    ref[pl.ds(at, block_rows), left : left + angles] = r
                    ref[pl.ds(at, block_rows), left + angles : left + 2 * angles] = m
                    ref[low, left : left + angles] = -m
                    ref[low, left + angles : left + 2 * angles] = r
                    real, imag = real - r.astype(jnp.float32), imag - m.astype(jnp.float32)
            return carry

        lax.fori_loop(0, angles // block_rows, strip, 0)

    def fold():
        form = form_ref[...]
        top = form.astype(LOW)
        low = (form - top.astype(jnp.float32)).astype(LOW)
        feats = form.shape[0]
        for child in range(2):
            hi, lo = base_hi[child], base_lo[child]
            value = low_dot(top, hi) + (low_dot(low, hi) + low_dot(top, lo))
            first = value.astype(LOW)
            at = slice(child * feats, (child + 1) * feats)
            fold_hi[at, :] = first
            fold_lo[at, :] = (value - first.astype(jnp.float32)).astype(LOW)

    def multiply(dz, dx, fresh):
        pair = flip(z, dz) * 2 + flip(x, dx)
        wide = 2 * chans * rows
        at = pl.multiple_of(pair * wide, wide)
        left = echo[:, :, :, :, pl.ds(at, wide)].reshape(-1, wide)
        right = jnp.concatenate([bg[0, pl.ds(at, wide), :], bg[1, pl.ds(at, wide), :]], axis=1)
        value = low_dot(left, right)
        acc[...] = value if fresh else acc[...] + value

    load_b.wait()
    other = pl.multiple_of((1 - c) * half, half)
    go(remote(bsrc.at[:, :, pl.ds(other, half)], ys, y_s, y_r, device(0, 0, 0, 1)))
    keep = pltpu.make_async_copy(piece(0, 0, 0), spot(0, 0, 0, 0), bz_r.at[0, 0, 0])
    keep.start()
    go(block(0, 1, 0))
    load_a.wait()
    pass_echo(0, (0, 0, 0), (1, 0, 0), (1, 0, 0, 0))
    pass_echo(1, (0, 0, 0), (0, 0, 1), (0, 0, 0, 1))
    far = [dz for dz in range(depth - 1, 0, -1)]
    for dz in far:
        for dk in range(2):
            go(block(dz, dk, 0))
    pass_echo(2, (0, 0, 0), (0, 1, 0), (0, 0, 1, 0))
    keep.wait()
    go(across(0, 0, 0))
    build(0, 0)
    arrived(0, 1, 0)
    go(across(0, 1, 0))
    build(0, 1)

    remote(ys, ys, y_s, y_r, device(0, 0, 0, 1)).wait_recv()
    keep = pltpu.make_async_copy(piece(0, 0, 1), spot(0, 0, 0, 1), bz_r.at[0, 0, 1])
    keep.start()
    go(block(0, 1, 1))
    for dz in far:
        for dk in range(2):
            go(block(dz, dk, 1))
    keep.wait()
    go(across(0, 0, 1))
    fold()
    arrived(0, 1, 1)
    go(across(0, 1, 1))

    pending = [(level, side) for level in range(1, levels) for side in range(2)]
    echo_in(1, 0, 0)
    pass_echo(3, (1, 0, 0), (1, 0, 1), (0, 0, 0, 1))
    pass_echo(4, (1, 0, 0), (1, 1, 0), (0, 0, 1, 0))
    for dz in far:
        for dk in range(2):
            arrived(dz, dk, 0)
            go(across(dz, dk, 0))
        if pending:
            build(*pending.pop(0))
    echo_in(0, 0, 1)
    pass_echo(5, (0, 0, 1), (0, 1, 1), (0, 0, 1, 0))
    for dz in far:
        for dk in range(2):
            arrived(dz, dk, 1)
            go(across(dz, dk, 1))
        if pending:
            build(*pending.pop(0))
    while pending:
        build(*pending.pop(0))
    echo_in(1, 0, 1)
    pass_echo(6, (1, 0, 1), (1, 1, 1), (0, 0, 1, 0))
    for da in range(2):
        for dc in range(2):
            echo_in(da, 1, dc)
    multiply(0, 0, True)
    for dz in far:
        multiply(dz, 0, False)
    for dz in [0] + far:
        for dk in range(2):
            for dc in range(2):
                crossed(dz, dk, dc)
        multiply(dz, 1, False)

    feats = form_ref.shape[0]
    value = acc[...].reshape(4, 2, feats // 2, 2 * LANES)
    for q in range(4):
        real = value[q, 0, :, :LANES] - value[q, 1, :, LANES:]
        imag = value[q, 0, :, LANES:] + value[q, 1, :, :LANES]
        turned = jnp.concatenate([real, imag], axis=0).T.astype(LOW)
        sbuf[:, q] = turned.reshape(group, own, feats)
    mine = zp * 2 + x
    spread = [(dzp, dx) for dzp in range(depth // 2 - 1, -1, -1) for dx in (1, 0)]
    for dzp, dx in spread:
        slot = dzp * 2 + dx
        if slot:
            to = flip(zp, dzp) * 2 + flip(x, dx)
            go(remote(sbuf.at[to], img0.at[mine], sb_s.at[slot], sb_r.at[slot], device(2 * dzp, dx, 0, 0)))
    img0[mine] = sbuf[mine]
    for dzp, dx in spread:
        slot = dzp * 2 + dx
        if slot:
            origin = flip(zp, dzp) * 2 + flip(x, dx)
            remote(
                sbuf.at[origin], img0.at[origin], sb_s.at[slot], sb_r.at[slot], device(2 * dzp, dx, 0, 0)
            ).wait_recv()

    place = (depth // 2, 2, 2, 2)
    wide = 2 * angles

    def child_rows(ref, axis, child, cols):
        split = (place[0] // 2, 2) + place[1:] if axis == 0 else place
        at = 1 if axis == 0 else axis
        whole = ref[...].reshape(split + (own, cols))
        return lax.index_in_dim(whole, child, at, keepdims=False).reshape(-1, cols)

    axis_of = [3, 1, 2] + [0] * (levels - 3)
    pair = jnp.concatenate([child_rows(img0, 3, child, feats) for child in range(2)], axis=1)
    source, target = img_a, img_b
    for side in range(2):
        cols = slice(side * wide, (side + 1) * wide)
        out = low_dot(pair, fold_hi[:, cols]) + low_dot(pair, fold_lo[:, cols])
        source[:, :, :, side] = out.astype(LOW).reshape(place[:3] + (own, wide))
    for level in range(1, levels - 1):
        first, second = (child_rows(source, axis_of[level], child, wide) for child in range(2))
        for side in range(2):
            cols = slice(side * wide, (side + 1) * wide)
            out = low_dot(first, ops[level - 1, 0, :, cols]) + low_dot(second, ops[level - 1, 1, :, cols])
            out = out.astype(LOW)
            if axis_of[level] == 1:
                target[:, side] = out.reshape(place[0], 2, 2, own, wide)
            else:
                target[:, :, side] = out.reshape(place[0], 2, 2, own, wide)
        source, target = target, source
    first, second = (child_rows(source, 0, child, wide) for child in range(2))
    base = HALO + (q_me * group + mine) * own
    block_at = pl.multiple_of(base, HALO)

    for turn in (1, 0):
        side = flip(zp, turn) % 2
        cols = pl.ds(pl.multiple_of(side * wide, wide), wide)
        out = low_dot(first, ops[levels - 2, 0, :, cols]) + low_dot(second, ops[levels - 2, 1, :, cols])
        power = out[:, :angles] * out[:, :angles] + out[:, angles:] * out[:, angles:]
        power = power.astype(LOW).reshape(place[0] // 2, 2, 2, 2, own, angles)
        for pair_at in range(place[0] // 2):
            pbuf[pair_at * 2 + side] = power[pair_at]
        for high in range(place[0] // 2):
            dzp = high * 2 + turn
            for rel in range(8):
                dx, dzz, dk = rel // 4, (rel // 2) % 2, rel % 2
                slot = dzp * 8 + rel
                src = pbuf.at[flip(zp, dzp), flip(x, dx), flip(par, dzz), flip(k, dk)]
                if slot:
                    go(
                        remote(
                            src,
                            rows_c.at[pl.ds(block_at, own), :],
                            sc_s.at[slot],
                            sc_r.at[slot],
                            device(2 * dzp + dzz, dx, dk, 0),
                        )
                    )

    def halo(slot, up):
        dzp, rel = slot // 8, slot % 8
        dx, dzz, dk = rel // 4, (rel // 2) % 2, rel % 2
        src = pbuf.at[flip(zp, dzp), flip(x, dx), flip(par, dzz), flip(k, dk)]
        src = src.at[pl.ds(own - HALO if up else 0, HALO), :]
        dst = rows_c.at[pl.ds(0 if up else HALO + half, HALO), :]
        return remote(src, dst, h_s.at[slot], h_r.at[0 if up else 1], device(2 * dzp + dzz, dx, dk, 1))

    order = list(range(subs - 1, -1, -1))
    sends_up = jnp.logical_and(c == 0, base == HALO + half - own)
    sends_down = jnp.logical_and(c == 1, base == HALO)

    @pl.when(sends_up)
    def _():
        for slot in order:
            halo(slot, True).start()

    @pl.when(sends_down)
    def _():
        for slot in order:
            halo(slot, False).start()

    rows_c[pl.ds(block_at, own), :] = pbuf[zp, x, par, k]

    @pl.when(c == 0)
    def _():
        rows_c[pl.ds(0, HALO), :] = jnp.zeros((HALO, angles), LOW)

    @pl.when(c == 1)
    def _():
        rows_c[pl.ds(HALO + half, HALO), :] = jnp.zeros((HALO, angles), LOW)

    for slot in order:
        if slot:
            dzp, rel = slot // 8, slot % 8
            dx, dzz, dk = rel // 4, (rel // 2) % 2, rel % 2
            origin = (flip(par, dzz) * 2 + flip(k, dk)) * group + flip(zp, dzp) * 2 + flip(x, dx)
            at = pl.multiple_of(HALO + origin * own, HALO)
            dst = rows_c.at[pl.ds(at, own), :]
            remote(
                dst, dst, sc_s.at[slot], sc_r.at[slot], device(2 * dzp + dzz, dx, dk, 0)
            ).wait_recv()

    @pl.when(c == 1)
    def _():
        halo(0, True).wait_recv()

    @pl.when(c == 0)
    def _():
        halo(0, False).wait_recv()

    out_ref[...] = rows_c[...]

    for copy in sent:
        copy.wait_send()

    @pl.when(sends_up)
    def _():
        for slot in order:
            halo(slot, True).wait_send()

    @pl.when(sends_down)
    def _():
        for slot in order:
            halo(slot, False).wait_send()


def smooth_body(chans, power_ref, rate_ref, out_ref):
    at = lax.axis_index("chan")
    power = power_ref[...].astype(jnp.float32)
    rate = rate_ref[...]
    height = power.shape[0] - 2 * HALO
    row = lax.broadcasted_iota(jnp.int32, power.shape, 0)
    inside = jnp.logical_and(
        jnp.logical_or(row >= HALO, at > 0), jnp.logical_or(row < HALO + height, at < chans - 1)
    )
    for sweep in range(PASSES):
        before = jnp.concatenate([power[:1], power[:-1]], axis=0)
        after = jnp.concatenate([power[1:], power[-1:]], axis=0)
        power = power + rate * (before - 2.0 * power + after)
        power = jnp.where(inside, power, 0.0)
    out_ref[...] = power[HALO : HALO + height].T


def local_kernel(
    raw_pulses, range_filter, channel_mix, steer_angles, band_offsets, band_weights, smoothing
):
    _, pulses, _, samples = raw_pulses.shape
    _, rows, bins = range_filter.shape
    angles = steer_angles.shape[0]
    levels, _, _, merged, band_width = band_weights.shape
    subs, chans = lax.axis_size("sub"), lax.axis_size("chan")
    half = bins // chans
    group = subs // 4
    own = LANES // group
    depth = subs // 4
    feats = 2 * chans * pulses
    form = forming_rows(channel_mix, steer_angles, pulses)
    place = (depth // 2, 2, 2, 2)
    dma = pltpu.SemaphoreType.DMA
    vmem = pl.BlockSpec(memory_space=pltpu.VMEM)
    anywhere = pl.BlockSpec(memory_space=pl.ANY)
    power = pl.pallas_call(
        functools.partial(window_body, subs),
        out_shape=jax.ShapeDtypeStruct((half + 2 * HALO, angles), LOW),
        in_specs=[anywhere, anywhere, vmem, vmem, vmem],
        out_specs=vmem,
        scratch_shapes=[
            pltpu.VMEM((2, rows, bins), LOW),
            pltpu.VMEM((2, rows, half), LOW),
            pltpu.VMEM((2, subs * chans * rows, LANES), LOW),
            pltpu.VMEM((4, 2, chans, pulses, samples), LOW),
            pltpu.VMEM((4 * feats, 2 * LANES), jnp.float32),
            pltpu.VMEM((2, 2 * angles, 2 * merged), LOW),
            pltpu.VMEM((2, 2 * angles, 2 * merged), LOW),
            pltpu.VMEM((2 * feats, 2 * merged), LOW),
            pltpu.VMEM((2 * feats, 2 * merged), LOW),
            pltpu.VMEM((levels - 1, 2, 2 * angles, 2 * merged), LOW),
            pltpu.VMEM((group, 4, own, feats), LOW),
            pltpu.VMEM((group, 4, own, feats), LOW),
            pltpu.VMEM(place + (own, 2 * angles), LOW),
            pltpu.VMEM(place + (own, 2 * angles), LOW),
            pltpu.VMEM(place + (own, angles), LOW),
            pltpu.VMEM((half + 2 * HALO, angles), LOW),
            dma((2,)),
            dma,
            dma,
            dma((depth, 2, 2)),
            dma((depth, 2, 2)),
            dma((depth, 2, 2)),
            dma((depth, 2, 2)),
            dma((7,)),
            dma((2, 2, 2)),
            dma((group,)),
            dma((group,)),
            dma((subs,)),
            dma((subs,)),
            dma((subs,)),
            dma((2,)),
        ],
        compiler_params=pltpu.CompilerParams(
            collective_id=0, has_side_effects=True, vmem_limit_bytes=56 << 20
        ),
    )(
        range_filter,
        raw_pulses[:, :, 0, :],
        form,
        band_offsets[:, None, :],
        band_weights.transpose(0, 1, 2, 4, 3),
    )
    return pl.pallas_call(
        functools.partial(smooth_body, chans),
        out_shape=jax.ShapeDtypeStruct((angles, half), jnp.float32),
        in_specs=[vmem, vmem],
        out_specs=vmem,
    )(power, smoothing[None, :])


def fits(mesh, raw_pulses, range_filter, steer_angles, band_offsets):
    subs, chans = mesh.shape["sub"], mesh.shape["chan"]
    rows = range_filter.shape[1] // (subs * chans)
    pulses = raw_pulses.shape[1] // subs
    cut = chans == 2 and subs % 16 == 0 and subs & (subs - 1) == 0
    cut = cut and range_filter.shape[2] == 4 * chans * LANES and LANES // (subs // 4) >= HALO
    cut = cut and rows % 16 == 0 and pulses % 16 == 0 and steer_angles.shape[0] % LANES == 0
    return cut and band_offsets.shape[0] == 4


def solution(mesh):
    in_specs = (
        P(None, "sub", "chan", None),
        P(None, ("sub", "chan"), None),
        P(),
        P(),
        P(),
        P(),
        P("sub"),
    )
    out_specs = P("sub", "chan")

    def run(raw_pulses, range_filter, channel_mix, steer_angles, band_offsets, band_weights, smoothing):
        one = local_kernel if fits(mesh, raw_pulses, range_filter, steer_angles, band_offsets) else local_plain
        part = jax.shard_map(one, mesh=mesh, in_specs=in_specs, out_specs=out_specs, check_vma=False)
        return part(
            raw_pulses, range_filter, channel_mix, steer_angles, band_offsets, band_weights, smoothing
        )

    return run
```

```python
import functools

import jax
import jax.numpy as jnp
import numpy as np
from jax import lax
from jax.experimental import pallas as pl
from jax.experimental.pallas import tpu as pltpu
from jax.sharding import PartitionSpec as P

PASSES = 3
HALO = 16
LANES = 128
HIGH = lax.Precision.HIGHEST
LOW = jnp.bfloat16
MESH = pl.DeviceIdType.MESH
def rounded(value):
    return lax.reduce_precision(value, exponent_bits=8, mantissa_bits=7)


def halves(value):
    top = rounded(value)
    return top.astype(LOW), (value - top).astype(LOW)


def doppler_table(count):
    index_row = jnp.arange(count, dtype=jnp.int32)
    product = index_row[:, None] * index_row[None, :] % count
    phase = 2.0 * np.pi / count * product.astype(jnp.float32)
    factor = 1.0 / np.sqrt(count)
    return (
        rounded(jnp.cos(phase) * factor),
        rounded(-jnp.sin(phase) * factor),
    )


def steer_table(steer_angles, count):
    offsets = jnp.arange(count, dtype=jnp.int32).astype(jnp.float32) - 0.5 * count
    phase = offsets[:, None] * steer_angles[None, :]
    factor = 1.0 / np.sqrt(count)
    return (
        rounded(jnp.cos(phase) * factor),
        rounded(jnp.sin(phase) * factor),
    )


def forming_operator(channel_mix, steer_angles, pulse_count):
    channels = channel_mix.shape[2]
    dop_r, dop_i = doppler_table(pulse_count)
    beam_r, beam_i = steer_table(steer_angles, channels * pulse_count)
    mix = channel_mix.transpose(0, 3, 2, 1)[:, :, None, :, :]
    dr, di = dop_r.T[None, :, None, :], dop_i.T[None, :, None, :]
    shape = (channels * pulse_count, channels * pulse_count)
    mixed_r = (mix[0] * dr - mix[1] * di).reshape(shape)
    mixed_i = (mix[0] * di + mix[1] * dr).reshape(shape)
    left = jnp.concatenate([mixed_r, mixed_i], axis=1)
    t_r = jnp.dot(left, jnp.concatenate([beam_r, -beam_i], axis=0), precision=HIGH)
    t_i = jnp.dot(left, jnp.concatenate([beam_i, beam_r], axis=0), precision=HIGH)
    angles = steer_angles.shape[0]
    t_r = t_r.reshape(channels, pulse_count, angles)
    t_i = t_i.reshape(channels, pulse_count, angles)
    top = jnp.concatenate([t_r, t_i], axis=2)
    low = jnp.concatenate([-t_i, t_r], axis=2)
    both = jnp.concatenate([top, low], axis=1)
    return both.reshape(channels * 2 * pulse_count, 2 * angles)


def operator_body(offsets_ref, weights_ref, *out_refs):
    band_width, count = weights_ref.shape[3], weights_ref.shape[4]
    delta = lax.broadcasted_iota(jnp.int32, (count, count), 0) - offsets_ref[0]
    bands = [jnp.zeros((count, count), jnp.float32)] * 2
    for j in range(band_width):
        hit = delta == j
        bands = [
            jnp.where(hit, weights_ref[0, 0, part, j : j + 1, :], bands[part]) for part in range(2)
        ]
    for order, ref in enumerate(out_refs):
        real, imag = (band.astype(LOW) for band in bands)
        ref[0, 0, :count, :count] = real
        ref[0, 0, :count, count:] = imag
        ref[0, 0, count:, :count] = -imag
        ref[0, 0, count:, count:] = real
        if order + 1 < len(out_refs):
            bands = [band - band.astype(LOW).astype(jnp.float32) for band in bands]


def merge_operators(offsets, weights, parts):
    levels, _, _, merged, band_width = weights.shape
    count = merged // 2
    by_step = weights.transpose(0, 1, 2, 4, 3)
    shape = jax.ShapeDtypeStruct((levels, 2, 2 * count, 2 * merged), LOW)
    return pl.pallas_call(
        operator_body,
        grid=(levels, 2, 2),
        in_specs=[
            pl.BlockSpec((1, 1, count), lambda l, c, h: (l, 0, h)),
            pl.BlockSpec((1, 1, 2, band_width, count), lambda l, c, h: (l, c, 0, 0, h)),
        ],
        out_specs=[
            pl.BlockSpec((1, 1, 2 * count, 2 * count), lambda l, c, h: (l, c, 0, h))
        ] * parts,
        out_shape=[shape] * parts,
        cost_estimate=pl.CostEstimate(
            flops=levels * 4 * count * count * 32,
            bytes_accessed=levels * parts * 16 * count * count * 2,
            transcendentals=0,
        ),
    )(offsets[:, None, :], by_step)


def low_dot(left, right):
    return jnp.dot(left, right, preferred_element_type=jnp.float32)


def local_plain(
    raw_pulses, range_filter, channel_mix, steer_angles, band_offsets, band_weights, smoothing
):
    pulses = raw_pulses.shape[1]
    samples = raw_pulses.shape[3]
    bins = range_filter.shape[2]
    angles = steer_angles.shape[0]
    levels = band_offsets.shape[0]
    subs, chans = lax.axis_size("sub"), lax.axis_size("chan")
    own = bins // (subs * chans)

    part = lax.all_to_all(range_filter, "chan", split_axis=2, concat_axis=1, tiled=True)
    filt = lax.all_gather(part, "sub", axis=1, tiled=True)
    echo = lax.all_gather(raw_pulses[:, :, 0, :], "chan", axis=0)

    forming = forming_operator(channel_mix, steer_angles, pulses)
    form_top, form_low = halves(forming)
    base_top, base_low = merge_operators(band_offsets[:1], band_weights[:1], 2)
    folded = [
        low_dot(form_top, base_top[0, c])
        + (low_dot(form_low, base_top[0, c]) + low_dot(form_top, base_low[0, c]))
        for c in range(2)
    ]
    folded_top, folded_low = halves(jnp.concatenate(folded, axis=0))
    (later,) = merge_operators(band_offsets[1:], band_weights[1:], 1)

    real_rows = jnp.concatenate([echo[:, 0], -echo[:, 1]], axis=2)
    imag_rows = jnp.concatenate([echo[:, 1], echo[:, 0]], axis=2)
    stacked = jnp.concatenate([real_rows, imag_rows], axis=1).reshape(-1, 2 * samples)
    compressed = low_dot(stacked, filt.reshape(2 * samples, -1)).astype(LOW)
    blocks = compressed.T.reshape(subs, own, -1)
    got = lax.all_to_all(blocks, "sub", split_axis=0, concat_axis=0, tiled=True)
    image = got.reshape(subs * own, -1)
    for level in range(levels):
        run = (1 << level) * own
        wide = image.shape[1]
        field = image.astype(LOW).reshape(-1, 2, run, wide)
        pair = jnp.concatenate([field[:, 0], field[:, 1]], axis=2).reshape(-1, 2 * wide)
        if level == 0:
            out = low_dot(pair, folded_top) + low_dot(pair, folded_low)
        else:
            out = low_dot(pair, later[level - 1].reshape(2 * wide, -1))
        out = out.reshape(-1, run, 4 * angles)
        image = jnp.stack([out[:, :, : 2 * angles], out[:, :, 2 * angles :]], axis=1)
        image = image.reshape(-1, 2 * angles)
    power = image[:, :angles] * image[:, :angles] + image[:, angles:] * image[:, angles:]
    power = power.astype(LOW).reshape(subs, own, angles)
    power = lax.all_to_all(power, "sub", split_axis=0, concat_axis=0, tiled=True)
    power = power.reshape(subs * own, angles)
    up = [(i, i + 1) for i in range(chans - 1)]
    down = [(j, i) for i, j in up]
    before = lax.ppermute(power[-PASSES:], "chan", up).astype(jnp.float32)
    after = lax.ppermute(power[:PASSES], "chan", down).astype(jnp.float32)
    power = jnp.concatenate([before, power.astype(jnp.float32), after], axis=0)
    rate = smoothing[None, :]
    at = lax.axis_index("chan")
    lead, trail = at == 0, at == chans - 1
    for sweep in range(PASSES):
        mid = power[1:-1]
        power = mid + rate * (power[:-2] - 2.0 * mid + power[2:])
        edge = PASSES - 1 - sweep
        if edge:
            inner = power[edge:-edge]
            head = jnp.where(lead, 0.0, power[:edge])
            tail = jnp.where(trail, 0.0, power[-edge:])
            power = jnp.concatenate([head, inner, tail], axis=0)
    return power.T


def narrow(value):
    return value.astype(LOW).astype(jnp.float32)


def high_dot(left, right):
    return jnp.dot(left, right, precision=HIGH, preferred_element_type=jnp.float32)


def flip(value, bits):
    out = value
    step = 1
    while step <= bits:
        if bits & step:
            out = out + step - 2 * step * ((value // step) % 2)
        step *= 2
    return out


def forming_rows(mix_ref, steer, pulse_count):
    bands, channels = mix_ref.shape[1], mix_ref.shape[2]
    angles = steer.shape[1]
    square = (pulse_count, pulse_count)
    product = lax.broadcasted_iota(jnp.int32, square, 0) * lax.broadcasted_iota(jnp.int32, square, 1)
    product = product.astype(jnp.float32)
    product = product - pulse_count * jnp.floor(product / pulse_count)
    phase = 2.0 * np.pi / pulse_count * product
    factor = 1.0 / np.sqrt(pulse_count)
    dop_r, dop_i = narrow(jnp.cos(phase) * factor), narrow(-jnp.sin(phase) * factor)
    count = channels * pulse_count
    factor = 1.0 / np.sqrt(count)
    t_r = t_i = None
    for band in range(bands):
        index = lax.broadcasted_iota(jnp.int32, (pulse_count, angles), 0) + band * pulse_count
        phase = (index.astype(jnp.float32) - 0.5 * count) * steer
        beam_r, beam_i = narrow(jnp.cos(phase) * factor), narrow(jnp.sin(phase) * factor)
        mixed = [[], []]
        for channel in range(channels):
            mix_r = mix_ref[0, band, channel : channel + 1, :]
            mix_i = mix_ref[1, band, channel : channel + 1, :]
            mixed[0].append(mix_r * dop_r - mix_i * dop_i)
            mixed[1].append(mix_r * dop_i + mix_i * dop_r)
        mixed_r, mixed_i = (jnp.concatenate(part, axis=0) for part in mixed)
        add_r = high_dot(mixed_r, beam_r) - high_dot(mixed_i, beam_i)
        add_i = high_dot(mixed_r, beam_i) + high_dot(mixed_i, beam_r)
        t_r = add_r if band == 0 else t_r + add_r
        t_i = add_i if band == 0 else t_i + add_i
    top = jnp.concatenate([t_r, t_i], axis=1)
    low = jnp.concatenate([-t_i, t_r], axis=1)
    return jnp.concatenate([top, low], axis=0)


def window_body(
    subs,
    filt_hbm,
    raw_hbm,
    mix_hbm,
    steer_hbm,
    offs_hbm,
    wts_hbm,
    out_ref,
    mix_ref,
    steer_ref,
    offs_ref,
    wts_ref,
    bsrc,
    ys,
    bg,
    echo,
    acc,
    base_hi,
    base_lo,
    fold_hi,
    fold_lo,
    ops,
    sbuf,
    img0,
    img_a,
    img_b,
    pbuf,
    rows_c,
    loc_sem,
    y_s,
    y_r,
    bz_s,
    bz_r,
    bx_s,
    bx_r,
    a_s,
    a_r,
    sb_s,
    sb_r,
    sc_s,
    sc_r,
    h_s,
    h_r,
    up_sem,
    down_sem,
):
    chans = 2
    rows = bsrc.shape[1]
    half = ys.shape[2]
    pulses = echo.shape[3]
    own = img0.shape[2]
    angles = steer_ref.shape[1]
    feats = 2 * chans * pulses
    depth = subs // 4
    group = subs // 4
    levels = offs_ref.shape[0]

    s, c = lax.axis_index("sub"), lax.axis_index("chan")
    z, x, k = s // 4, (s // 2) % 2, s % 2
    par, zp = z % 2, z // 2

    def sub_at(dz, dx, dk):
        return flip(z, dz) * 4 + flip(x, dx) * 2 + flip(k, dk)

    def device(dz, dx, dk, dc):
        return {"sub": sub_at(dz, dx, dk), "chan": flip(c, dc)}

    def remote(src, dst, send, recv, dev):
        return pltpu.make_async_remote_copy(
            src_ref=src, dst_ref=dst, send_sem=send, recv_sem=recv, device_id=dev, device_id_type=MESH
        )

    q_me = par * 2 + k
    load_b = pltpu.make_async_copy(filt_hbm, bsrc, loc_sem.at[0])
    load_a = pltpu.make_async_copy(raw_hbm, echo.at[q_me, :, c], loc_sem.at[1])
    tables = [
        pltpu.make_async_copy(src, dst, loc_sem.at[2 + i])
        for i, (src, dst) in enumerate(
            [(offs_hbm, offs_ref), (wts_hbm, wts_ref), (mix_hbm, mix_ref), (steer_hbm, steer_ref)]
        )
    ]
    load_b.start()
    load_a.start()
    for table in tables:
        table.start()

    barrier = pltpu.get_barrier_semaphore()

    def greet(sub, chan):
        pl.semaphore_signal(barrier, inc=1, device_id={"sub": sub, "chan": chan}, device_id_type=MESH)

    def along(step, dk):
        return (z + step) * 4 + x * 2 + flip(k, dk)

    greet(s, 1 - c)
    greet(sub_at(0, 1, 0), c)
    greet(sub_at(0, 0, 1), c)
    below, above = z > 0, z < depth - 1

    @pl.when(below)
    def _():
        greet(along(-1, 0), c)
        greet(along(-1, 1), c)

    @pl.when(above)
    def _():
        greet(along(1, 0), c)
        greet(along(1, 1), c)

    pl.semaphore_wait(barrier, 3 + 2 * lax.min(z, 1) + 2 * lax.min(depth - 1 - z, 1))

    def tell(step, far, sem):
        pl.semaphore_signal(sem, inc=1, device_id={"sub": along(step, 0), "chan": c}, device_id_type=MESH)

    def spread_word(far):
        @pl.when(jnp.logical_and(below, z + far - 1 < depth))
        def _():
            tell(-1, far, up_sem.at[far - 2])

        @pl.when(jnp.logical_and(above, z - far + 1 >= 0))
        def _():
            tell(1, far, down_sem.at[far - 2])

        @pl.when(z + far < depth)
        def _():
            pl.semaphore_wait(up_sem.at[far - 2], 1)

        @pl.when(z - far >= 0)
        def _():
            pl.semaphore_wait(down_sem.at[far - 2], 1)

    sent = []

    def go(copy):
        copy.start()
        sent.append(copy)

    inner = (z + zp) % 2

    def reach(turn):
        if turn == 0:
            return z, 0
        if turn == 1:
            return flip(z, 1), 1
        if turn == 2:
            return depth // 2 - zp, 2 + inner
        return (depth - 1) * (1 - zp), 3 - inner

    def spot(at_z, dx, dk, dc):
        at = ((at_z * 4 + flip(x, dx) * 2 + flip(k, dk)) * chans + flip(c, dc)) * rows
        return bg.at[:, pl.ds(pl.multiple_of(at, rows), rows), :]

    def piece(at_z, dk, dc):
        column = ((at_z % 2) * 2 + flip(k, dk)) * LANES
        if dc:
            return ys.at[:, :, pl.ds(pl.multiple_of(column, LANES), LANES)]
        return bsrc.at[:, :, pl.ds(pl.multiple_of(c * half + column, LANES), LANES)]

    def block(turn, dk, dc):
        at_z, bits = reach(turn)
        to = {"sub": at_z * 4 + x * 2 + flip(k, dk), "chan": c}
        return remote(piece(at_z, dk, dc), spot(z, 0, 0, dc), bz_s.at[turn, dk, dc], bz_r.at[bits, dk, dc], to)

    def keep(dc):
        copy = pltpu.make_async_copy(piece(z, 0, dc), spot(z, 0, 0, dc), bz_r.at[0, 0, dc])
        copy.start()
        return copy

    def arrived(turn, dk, dc):
        at_z, bits = reach(turn)
        here = spot(at_z, 0, dk, dc)
        remote(here, here, bz_s.at[turn, dk, dc], bz_r.at[bits, dk, dc], device(0, 1, 0, 0)).wait_recv()

    def across(turn, dk, dc):
        at_z, bits = reach(turn)
        here = spot(at_z, 0, dk, dc)
        return remote(here, here, bx_s.at[turn, dk, dc], bx_r.at[bits, dk, dc], device(0, 1, 0, 0))

    def crossed(turn, dk, dc):
        at_z, bits = reach(turn)
        there = spot(at_z, 1, dk, dc)
        remote(there, there, bx_s.at[turn, dk, dc], bx_r.at[bits, dk, dc], device(0, 1, 0, 0)).wait_recv()

    def echo_at(da, dk, dc, part):
        return echo.at[flip(par, da) * 2 + flip(k, dk), part, flip(c, dc)]

    def pass_echo(slot, here, there, dev, part):
        spot_here = echo_at(*here, part)
        go(remote(spot_here, spot_here, a_s.at[slot, part], a_r.at[there + (part,)], device(*dev)))

    def echo_in(da, dk, dc, part):
        there = echo_at(da, dk, dc, part)
        remote(there, there, a_s.at[0, part], a_r.at[da, dk, dc, part], device(0, 0, 0, 1)).wait_recv()

    def build(level, side):
        block_rows = 32
        lane = side * angles
        offs = offs_ref[level : level + 1, lane : lane + angles]

        def strip(i, carry):
            at = pl.multiple_of(i * block_rows, block_rows)
            delta = lax.broadcasted_iota(jnp.int32, (block_rows, angles), 0) + at - offs
            band = [[jnp.zeros((block_rows, angles), jnp.float32)] * 2 for _ in range(2)]
            for j in range(wts_ref.shape[3]):
                hit = delta == j
                for child in range(2):
                    for part in range(2):
                        row = wts_ref[level, child, part, j : j + 1, lane : lane + angles]
                        band[child][part] = jnp.where(hit, row, band[child][part])
            left = 2 * lane
            for child in range(2):
                real, imag = band[child]
                for order in range(2 if level == 0 else 1):
                    r, m = real.astype(LOW), imag.astype(LOW)
                    if level == 0:
                        ref = (base_hi if order == 0 else base_lo).at[child]
                    else:
                        ref = ops.at[level - 1, child]
                    low = pl.ds(pl.multiple_of(angles + at, block_rows), block_rows)
                    ref[pl.ds(at, block_rows), left : left + angles] = r
                    ref[pl.ds(at, block_rows), left + angles : left + 2 * angles] = m
                    ref[low, left : left + angles] = -m
                    ref[low, left + angles : left + 2 * angles] = r
                    real, imag = real - r.astype(jnp.float32), imag - m.astype(jnp.float32)
            return carry

        lax.fori_loop(0, angles // block_rows, strip, 0)

    def fold():
        form = forming_rows(mix_ref, steer_ref[...], pulses)
        top = form.astype(LOW)
        low = (form - top.astype(jnp.float32)).astype(LOW)
        for child in range(2):
            hi, lo = base_hi[child], base_lo[child]
            value = low_dot(top, hi) + (low_dot(low, hi) + low_dot(top, lo))
            first = value.astype(LOW)
            at = slice(child * feats, (child + 1) * feats)
            fold_hi[at, :] = first
            fold_lo[at, :] = (value - first.astype(jnp.float32)).astype(LOW)

    def multiply(turn, dx, fresh):
        pair = reach(turn)[0] * 2 + flip(x, dx)
        wide = 2 * chans * rows
        at = pl.multiple_of(pair * wide, wide)
        left = echo[:, :, :, :, pl.ds(at, wide)].reshape(-1, wide)
        right = jnp.concatenate([bg[0, pl.ds(at, wide), :], bg[1, pl.ds(at, wide), :]], axis=1)
        value = low_dot(left, right)
        acc[...] = value if fresh else acc[...] + value

    load_b.wait()
    other = pl.multiple_of((1 - c) * half, half)
    go(remote(bsrc.at[:, :, pl.ds(other, half)], ys, y_s, y_r, device(0, 0, 0, 1)))
    kept = keep(0)
    go(block(0, 1, 0))
    load_a.wait()
    pass_echo(0, (0, 0, 0), (1, 0, 0), (1, 0, 0, 0), 0)
    for part in range(2):
        pass_echo(1, (0, 0, 0), (0, 0, 1), (0, 0, 0, 1), part)
    for dk in range(2):
        go(block(1, dk, 0))
    for part in range(2):
        pass_echo(2, (0, 0, 0), (0, 1, 0), (0, 0, 1, 0), part)
    far_pairs = [block(turn, dk, 0) for turn in range(2, depth) for dk in range(2)]
    sent.extend(far_pairs)

    @pl.when(inner == 1)
    def _():
        for copy in far_pairs[:2]:
            copy.start()

    kept.wait()
    go(across(0, 0, 0))
    spread_word(2)

    @pl.when(inner == 1)
    def _():
        for copy in far_pairs[2:]:
            copy.start()

    @pl.when(inner == 0)
    def _():
        for copy in far_pairs[:2]:
            copy.start()

    arrived(0, 1, 0)
    go(across(0, 1, 0))
    spread_word(3)

    @pl.when(inner == 0)
    def _():
        for copy in far_pairs[2:]:
            copy.start()

    pass_echo(0, (0, 0, 0), (1, 0, 0), (1, 0, 0, 0), 1)

    remote(ys, ys, y_s, y_r, device(0, 0, 0, 1)).wait_recv()
    kept = keep(1)
    go(block(0, 1, 1))
    for dk in range(2):
        for turn in range(1, depth):
            go(block(turn, dk, 1))
    kept.wait()
    go(across(0, 0, 1))
    for table in tables:
        table.wait()
    pending = [(level, side) for level in range(levels) for side in range(2)]
    build(*pending.pop(0))

    def relay(part):
        echo_in(1, 0, 0, part)
        pass_echo(3, (1, 0, 0), (1, 0, 1), (0, 0, 0, 1), part)
        pass_echo(4, (1, 0, 0), (1, 1, 0), (0, 0, 1, 0), part)

    relay(0)
    arrived(0, 1, 1)
    go(across(0, 1, 1))
    for dc in range(2):
        for dk in range(2):
            for turn in range(1, depth):
                arrived(turn, dk, dc)
                go(across(turn, dk, dc))
            if pending:
                build(*pending.pop(0))
            if dc == 0 and dk == 1:
                fold()
        if dc == 0:
            relay(1)
            for part in range(2):
                echo_in(0, 0, 1, part)
                pass_echo(5, (0, 0, 1), (0, 1, 1), (0, 0, 1, 0), part)
    for part in range(2):
        echo_in(1, 0, 1, part)
        pass_echo(6, (1, 0, 1), (1, 1, 1), (0, 0, 1, 0), part)
    while pending:
        build(*pending.pop(0))
    for da in range(2):
        for dc in range(2):
            for part in range(2):
                echo_in(da, 1, dc, part)
    multiply(0, 0, True)
    for turn in range(1, depth):
        multiply(turn, 0, False)
    for turn in range(depth):
        for dk in range(2):
            for dc in range(2):
                crossed(turn, dk, dc)
        multiply(turn, 1, False)

    value = acc[...].reshape(4, 2, feats // 2, 2 * LANES)
    for q in range(4):
        real = value[q, 0, :, :LANES] - value[q, 1, :, LANES:]
        imag = value[q, 0, :, LANES:] + value[q, 1, :, :LANES]
        turned = jnp.concatenate([real, imag], axis=0).T.astype(LOW)
        sbuf[:, q] = turned.reshape(group, own, feats)
    mine = zp * 2 + x
    spread = [(dzp, dx) for dzp in range(depth // 2 - 1, -1, -1) for dx in (1, 0)]
    for dzp, dx in spread:
        slot = dzp * 2 + dx
        if slot:
            to = flip(zp, dzp) * 2 + flip(x, dx)
            go(remote(sbuf.at[to], img0.at[mine], sb_s.at[slot], sb_r.at[slot], device(2 * dzp, dx, 0, 0)))
    img0[mine] = sbuf[mine]
    for dzp, dx in spread:
        slot = dzp * 2 + dx
        if slot:
            origin = flip(zp, dzp) * 2 + flip(x, dx)
            remote(
                sbuf.at[origin], img0.at[origin], sb_s.at[slot], sb_r.at[slot], device(2 * dzp, dx, 0, 0)
            ).wait_recv()

    place = (depth // 2, 2, 2, 2)
    wide = 2 * angles

    def child_rows(ref, axis, child, cols):
        split = (place[0] // 2, 2) + place[1:] if axis == 0 else place
        at = 1 if axis == 0 else axis
        whole = ref[...].reshape(split + (own, cols))
        return lax.index_in_dim(whole, child, at, keepdims=False).reshape(-1, cols)

    axis_of = [3, 1, 2] + [0] * (levels - 3)
    pair = jnp.concatenate([child_rows(img0, 3, child, feats) for child in range(2)], axis=1)
    source, target = img_a, img_b
    for side in range(2):
        cols = slice(side * wide, (side + 1) * wide)
        out = low_dot(pair, fold_hi[:, cols]) + low_dot(pair, fold_lo[:, cols])
        source[:, :, :, side] = out.astype(LOW).reshape(place[:3] + (own, wide))
    for level in range(1, levels - 1):
        first, second = (child_rows(source, axis_of[level], child, wide) for child in range(2))
        for side in range(2):
            cols = slice(side * wide, (side + 1) * wide)
            out = low_dot(first, ops[level - 1, 0, :, cols]) + low_dot(second, ops[level - 1, 1, :, cols])
            out = out.astype(LOW)
            if axis_of[level] == 1:
                target[:, side] = out.reshape(place[0], 2, 2, own, wide)
            else:
                target[:, :, side] = out.reshape(place[0], 2, 2, own, wide)
        source, target = target, source
    first, second = (child_rows(source, 0, child, wide) for child in range(2))
    base = HALO + (q_me * group + mine) * own
    block_at = pl.multiple_of(base, HALO)

    for turn in (1, 0):
        side = flip(zp, turn) % 2
        cols = pl.ds(pl.multiple_of(side * wide, wide), wide)
        out = low_dot(first, ops[levels - 2, 0, :, cols]) + low_dot(second, ops[levels - 2, 1, :, cols])
        power = out[:, :angles] * out[:, :angles] + out[:, angles:] * out[:, angles:]
        power = power.astype(LOW).reshape(place[0] // 2, 2, 2, 2, own, angles)
        for pair_at in range(place[0] // 2):
            pbuf[pair_at * 2 + side] = power[pair_at]
        for high in range(place[0] // 2):
            dzp = high * 2 + turn
            for rel in range(8):
                dx, dzz, dk = rel // 4, (rel // 2) % 2, rel % 2
                slot = dzp * 8 + rel
                src = pbuf.at[flip(zp, dzp), flip(x, dx), flip(par, dzz), flip(k, dk)]
                if slot:
                    go(
                        remote(
                            src,
                            rows_c.at[pl.ds(block_at, own), :],
                            sc_s.at[slot],
                            sc_r.at[slot],
                            device(2 * dzp + dzz, dx, dk, 0),
                        )
                    )

    def halo(slot, up):
        dzp, rel = slot // 8, slot % 8
        dx, dzz, dk = rel // 4, (rel // 2) % 2, rel % 2
        src = pbuf.at[flip(zp, dzp), flip(x, dx), flip(par, dzz), flip(k, dk)]
        src = src.at[pl.ds(own - HALO if up else 0, HALO), :]
        dst = rows_c.at[pl.ds(0 if up else HALO + half, HALO), :]
        return remote(src, dst, h_s.at[slot], h_r.at[0 if up else 1], device(2 * dzp + dzz, dx, dk, 1))

    order = list(range(subs - 1, -1, -1))
    sends_up = jnp.logical_and(c == 0, base == HALO + half - own)
    sends_down = jnp.logical_and(c == 1, base == HALO)

    @pl.when(sends_up)
    def _():
        for slot in order:
            halo(slot, True).start()

    @pl.when(sends_down)
    def _():
        for slot in order:
            halo(slot, False).start()

    rows_c[pl.ds(block_at, own), :] = pbuf[zp, x, par, k]

    @pl.when(c == 0)
    def _():
        rows_c[pl.ds(0, HALO), :] = jnp.zeros((HALO, angles), LOW)

    @pl.when(c == 1)
    def _():
        rows_c[pl.ds(HALO + half, HALO), :] = jnp.zeros((HALO, angles), LOW)

    for slot in order:
        if slot:
            dzp, rel = slot // 8, slot % 8
            dx, dzz, dk = rel // 4, (rel // 2) % 2, rel % 2
            origin = (flip(par, dzz) * 2 + flip(k, dk)) * group + flip(zp, dzp) * 2 + flip(x, dx)
            at = pl.multiple_of(HALO + origin * own, HALO)
            dst = rows_c.at[pl.ds(at, own), :]
            remote(
                dst, dst, sc_s.at[slot], sc_r.at[slot], device(2 * dzp + dzz, dx, dk, 0)
            ).wait_recv()

    @pl.when(c == 1)
    def _():
        halo(0, True).wait_recv()

    @pl.when(c == 0)
    def _():
        halo(0, False).wait_recv()

    out_ref[...] = rows_c[...]

    for copy in sent:
        copy.wait_send()

    @pl.when(sends_up)
    def _():
        for slot in order:
            halo(slot, True).wait_send()

    @pl.when(sends_down)
    def _():
        for slot in order:
            halo(slot, False).wait_send()


def smooth_body(chans, power_ref, rate_ref, out_ref):
    at = lax.axis_index("chan")
    power = power_ref[...].astype(jnp.float32)
    rate = rate_ref[...]
    height = power.shape[0] - 2 * HALO
    row = lax.broadcasted_iota(jnp.int32, power.shape, 0)
    inside = jnp.logical_and(
        jnp.logical_or(row >= HALO, at > 0), jnp.logical_or(row < HALO + height, at < chans - 1)
    )
    for sweep in range(PASSES):
        before = jnp.concatenate([power[:1], power[:-1]], axis=0)
        after = jnp.concatenate([power[1:], power[-1:]], axis=0)
        power = power + rate * (before - 2.0 * power + after)
        power = jnp.where(inside, power, 0.0)
    out_ref[...] = power[HALO : HALO + height].T


def local_kernel(
    raw_pulses, range_filter, channel_mix, steer_angles, band_offsets, band_weights, smoothing
):
    _, pulses, _, samples = raw_pulses.shape
    _, rows, bins = range_filter.shape
    angles = steer_angles.shape[0]
    levels, _, _, merged, band_width = band_weights.shape
    subs, chans = lax.axis_size("sub"), lax.axis_size("chan")
    half = bins // chans
    group = subs // 4
    own = LANES // group
    depth = subs // 4
    feats = 2 * chans * pulses
    place = (depth // 2, 2, 2, 2)
    dma = pltpu.SemaphoreType.DMA
    vmem = pl.BlockSpec(memory_space=pltpu.VMEM)
    anywhere = pl.BlockSpec(memory_space=pl.ANY)
    power = pl.pallas_call(
        functools.partial(window_body, subs),
        out_shape=jax.ShapeDtypeStruct((half + 2 * HALO, angles), LOW),
        in_specs=[pl.BlockSpec(memory_space=pltpu.HBM)] * 6,
        out_specs=vmem,
        scratch_shapes=[
            pltpu.VMEM((2, chans, chans, pulses), jnp.float32),
            pltpu.VMEM((1, angles), jnp.float32),
            pltpu.VMEM((levels, merged), jnp.int32),
            pltpu.VMEM((levels, 2, 2, band_width, merged), jnp.float32),
            pltpu.VMEM((2, rows, bins), LOW),
            pltpu.VMEM((2, rows, half), LOW),
            pltpu.VMEM((2, subs * chans * rows, LANES), LOW),
            pltpu.VMEM((4, 2, chans, pulses, samples), LOW),
            pltpu.VMEM((4 * feats, 2 * LANES), jnp.float32),
            pltpu.VMEM((2, 2 * angles, 2 * merged), LOW),
            pltpu.VMEM((2, 2 * angles, 2 * merged), LOW),
            pltpu.VMEM((2 * feats, 2 * merged), LOW),
            pltpu.VMEM((2 * feats, 2 * merged), LOW),
            pltpu.VMEM((levels - 1, 2, 2 * angles, 2 * merged), LOW),
            pltpu.VMEM((group, 4, own, feats), LOW),
            pltpu.VMEM((group, 4, own, feats), LOW),
            pltpu.VMEM(place + (own, 2 * angles), LOW),
            pltpu.VMEM(place + (own, 2 * angles), LOW),
            pltpu.VMEM(place + (own, angles), LOW),
            pltpu.VMEM((half + 2 * HALO, angles), LOW),
            dma((6,)),
            dma,
            dma,
            dma((depth, 2, 2)),
            dma((depth, 2, 2)),
            dma((depth, 2, 2)),
            dma((depth, 2, 2)),
            dma((7, 2)),
            dma((2, 2, 2, 2)),
            dma((group,)),
            dma((group,)),
            dma((subs,)),
            dma((subs,)),
            dma((subs,)),
            dma((2,)),
            pltpu.SemaphoreType.REGULAR((depth - 2,)),
            pltpu.SemaphoreType.REGULAR((depth - 2,)),
        ],
        compiler_params=pltpu.CompilerParams(
            collective_id=0, has_side_effects=True, vmem_limit_bytes=32 << 20
        ),
    )(
        *(
            pltpu.with_memory_space_constraint(array, pltpu.HBM)
            for array in (
                range_filter,
                raw_pulses[:, :, 0, :],
                channel_mix.transpose(0, 2, 3, 1),
                steer_angles[None, :],
                band_offsets,
                band_weights.transpose(0, 1, 2, 4, 3),
            )
        )
    )
    return pl.pallas_call(
        functools.partial(smooth_body, chans),
        out_shape=jax.ShapeDtypeStruct((angles, half), jnp.float32),
        in_specs=[vmem, vmem],
        out_specs=vmem,
        compiler_params=pltpu.CompilerParams(vmem_limit_bytes=8 << 20),
    )(power, smoothing[None, :])


def fits(mesh, raw_pulses, range_filter, steer_angles, band_offsets):
    subs, chans = mesh.shape["sub"], mesh.shape["chan"]
    rows = range_filter.shape[1] // (subs * chans)
    pulses = raw_pulses.shape[1] // subs
    cut = chans == 2 and subs // 4 == 4
    cut = cut and range_filter.shape[2] == 4 * chans * LANES and LANES // (subs // 4) >= HALO
    cut = cut and rows % 16 == 0 and pulses % 16 == 0 and steer_angles.shape[0] % LANES == 0
    return cut and band_offsets.shape[0] == 4


def solution(mesh):
    in_specs = (
        P(None, "sub", "chan", None),
        P(None, ("sub", "chan"), None),
        P(),
        P(),
        P(),
        P(),
        P("sub"),
    )
    out_specs = P("sub", "chan")

    def run(raw_pulses, range_filter, channel_mix, steer_angles, band_offsets, band_weights, smoothing):
        one = local_kernel if fits(mesh, raw_pulses, range_filter, steer_angles, band_offsets) else local_plain
        part = jax.shard_map(one, mesh=mesh, in_specs=in_specs, out_specs=out_specs, check_vma=False)
        return part(
            raw_pulses, range_filter, channel_mix, steer_angles, band_offsets, band_weights, smoothing
        )

    return run
```

```python
import functools

import jax
import jax.numpy as jnp
import numpy as np
from jax import lax
from jax.experimental import pallas as pl
from jax.experimental.pallas import tpu as pltpu
from jax.sharding import PartitionSpec as P

PASSES = 3
HALO = 16
LANES = 128
HIGH = lax.Precision.HIGHEST
LOW = jnp.bfloat16
MESH = pl.DeviceIdType.MESH
def rounded(value):
    return lax.reduce_precision(value, exponent_bits=8, mantissa_bits=7)


def halves(value):
    top = rounded(value)
    return top.astype(LOW), (value - top).astype(LOW)


def doppler_table(count):
    index_row = jnp.arange(count, dtype=jnp.int32)
    product = index_row[:, None] * index_row[None, :] % count
    phase = 2.0 * np.pi / count * product.astype(jnp.float32)
    factor = 1.0 / np.sqrt(count)
    return (
        rounded(jnp.cos(phase) * factor),
        rounded(-jnp.sin(phase) * factor),
    )


def steer_table(steer_angles, count):
    offsets = jnp.arange(count, dtype=jnp.int32).astype(jnp.float32) - 0.5 * count
    phase = offsets[:, None] * steer_angles[None, :]
    factor = 1.0 / np.sqrt(count)
    return (
        rounded(jnp.cos(phase) * factor),
        rounded(jnp.sin(phase) * factor),
    )


def forming_operator(channel_mix, steer_angles, pulse_count):
    channels = channel_mix.shape[2]
    dop_r, dop_i = doppler_table(pulse_count)
    beam_r, beam_i = steer_table(steer_angles, channels * pulse_count)
    mix = channel_mix.transpose(0, 3, 2, 1)[:, :, None, :, :]
    dr, di = dop_r.T[None, :, None, :], dop_i.T[None, :, None, :]
    shape = (channels * pulse_count, channels * pulse_count)
    mixed_r = (mix[0] * dr - mix[1] * di).reshape(shape)
    mixed_i = (mix[0] * di + mix[1] * dr).reshape(shape)
    left = jnp.concatenate([mixed_r, mixed_i], axis=1)
    t_r = jnp.dot(left, jnp.concatenate([beam_r, -beam_i], axis=0), precision=HIGH)
    t_i = jnp.dot(left, jnp.concatenate([beam_i, beam_r], axis=0), precision=HIGH)
    angles = steer_angles.shape[0]
    t_r = t_r.reshape(channels, pulse_count, angles)
    t_i = t_i.reshape(channels, pulse_count, angles)
    top = jnp.concatenate([t_r, t_i], axis=2)
    low = jnp.concatenate([-t_i, t_r], axis=2)
    both = jnp.concatenate([top, low], axis=1)
    return both.reshape(channels * 2 * pulse_count, 2 * angles)


def operator_body(offsets_ref, weights_ref, *out_refs):
    band_width, count = weights_ref.shape[3], weights_ref.shape[4]
    delta = lax.broadcasted_iota(jnp.int32, (count, count), 0) - offsets_ref[0]
    bands = [jnp.zeros((count, count), jnp.float32)] * 2
    for j in range(band_width):
        hit = delta == j
        bands = [
            jnp.where(hit, weights_ref[0, 0, part, j : j + 1, :], bands[part]) for part in range(2)
        ]
    for order, ref in enumerate(out_refs):
        real, imag = (band.astype(LOW) for band in bands)
        ref[0, 0, :count, :count] = real
        ref[0, 0, :count, count:] = imag
        ref[0, 0, count:, :count] = -imag
        ref[0, 0, count:, count:] = real
        if order + 1 < len(out_refs):
            bands = [band - band.astype(LOW).astype(jnp.float32) for band in bands]


def merge_operators(offsets, weights, parts):
    levels, _, _, merged, band_width = weights.shape
    count = merged // 2
    by_step = weights.transpose(0, 1, 2, 4, 3)
    shape = jax.ShapeDtypeStruct((levels, 2, 2 * count, 2 * merged), LOW)
    return pl.pallas_call(
        operator_body,
        grid=(levels, 2, 2),
        in_specs=[
            pl.BlockSpec((1, 1, count), lambda l, c, h: (l, 0, h)),
            pl.BlockSpec((1, 1, 2, band_width, count), lambda l, c, h: (l, c, 0, 0, h)),
        ],
        out_specs=[
            pl.BlockSpec((1, 1, 2 * count, 2 * count), lambda l, c, h: (l, c, 0, h))
        ] * parts,
        out_shape=[shape] * parts,
        cost_estimate=pl.CostEstimate(
            flops=levels * 4 * count * count * 32,
            bytes_accessed=levels * parts * 16 * count * count * 2,
            transcendentals=0,
        ),
    )(offsets[:, None, :], by_step)


def low_dot(left, right):
    return jnp.dot(left, right, preferred_element_type=jnp.float32)


def local_plain(
    raw_pulses, range_filter, channel_mix, steer_angles, band_offsets, band_weights, smoothing
):
    pulses = raw_pulses.shape[1]
    samples = raw_pulses.shape[3]
    bins = range_filter.shape[2]
    angles = steer_angles.shape[0]
    levels = band_offsets.shape[0]
    subs, chans = lax.axis_size("sub"), lax.axis_size("chan")
    own = bins // (subs * chans)

    part = lax.all_to_all(range_filter, "chan", split_axis=2, concat_axis=1, tiled=True)
    filt = lax.all_gather(part, "sub", axis=1, tiled=True)
    echo = lax.all_gather(raw_pulses[:, :, 0, :], "chan", axis=0)

    forming = forming_operator(channel_mix, steer_angles, pulses)
    form_top, form_low = halves(forming)
    base_top, base_low = merge_operators(band_offsets[:1], band_weights[:1], 2)
    folded = [
        low_dot(form_top, base_top[0, c])
        + (low_dot(form_low, base_top[0, c]) + low_dot(form_top, base_low[0, c]))
        for c in range(2)
    ]
    folded_top, folded_low = halves(jnp.concatenate(folded, axis=0))
    (later,) = merge_operators(band_offsets[1:], band_weights[1:], 1)

    real_rows = jnp.concatenate([echo[:, 0], -echo[:, 1]], axis=2)
    imag_rows = jnp.concatenate([echo[:, 1], echo[:, 0]], axis=2)
    stacked = jnp.concatenate([real_rows, imag_rows], axis=1).reshape(-1, 2 * samples)
    compressed = low_dot(stacked, filt.reshape(2 * samples, -1)).astype(LOW)
    blocks = compressed.T.reshape(subs, own, -1)
    got = lax.all_to_all(blocks, "sub", split_axis=0, concat_axis=0, tiled=True)
    image = got.reshape(subs * own, -1)
    for level in range(levels):
        run = (1 << level) * own
        wide = image.shape[1]
        field = image.astype(LOW).reshape(-1, 2, run, wide)
        pair = jnp.concatenate([field[:, 0], field[:, 1]], axis=2).reshape(-1, 2 * wide)
        if level == 0:
            out = low_dot(pair, folded_top) + low_dot(pair, folded_low)
        else:
            out = low_dot(pair, later[level - 1].reshape(2 * wide, -1))
        out = out.reshape(-1, run, 4 * angles)
        image = jnp.stack([out[:, :, : 2 * angles], out[:, :, 2 * angles :]], axis=1)
        image = image.reshape(-1, 2 * angles)
    power = image[:, :angles] * image[:, :angles] + image[:, angles:] * image[:, angles:]
    power = power.astype(LOW).reshape(subs, own, angles)
    power = lax.all_to_all(power, "sub", split_axis=0, concat_axis=0, tiled=True)
    power = power.reshape(subs * own, angles)
    up = [(i, i + 1) for i in range(chans - 1)]
    down = [(j, i) for i, j in up]
    before = lax.ppermute(power[-PASSES:], "chan", up).astype(jnp.float32)
    after = lax.ppermute(power[:PASSES], "chan", down).astype(jnp.float32)
    power = jnp.concatenate([before, power.astype(jnp.float32), after], axis=0)
    rate = smoothing[None, :]
    at = lax.axis_index("chan")
    lead, trail = at == 0, at == chans - 1
    for sweep in range(PASSES):
        mid = power[1:-1]
        power = mid + rate * (power[:-2] - 2.0 * mid + power[2:])
        edge = PASSES - 1 - sweep
        if edge:
            inner = power[edge:-edge]
            head = jnp.where(lead, 0.0, power[:edge])
            tail = jnp.where(trail, 0.0, power[-edge:])
            power = jnp.concatenate([head, inner, tail], axis=0)
    return power.T


def narrow(value):
    return value.astype(LOW).astype(jnp.float32)


def high_dot(left, right):
    return jnp.dot(left, right, precision=HIGH, preferred_element_type=jnp.float32)


def flip(value, bits):
    out = value
    step = 1
    while step <= bits:
        if bits & step:
            out = out + step - 2 * step * ((value // step) % 2)
        step *= 2
    return out


def forming_rows(mix_ref, steer, pulse_count):
    bands, channels = mix_ref.shape[1], mix_ref.shape[2]
    angles = steer.shape[1]
    square = (pulse_count, pulse_count)
    product = lax.broadcasted_iota(jnp.int32, square, 0) * lax.broadcasted_iota(jnp.int32, square, 1)
    product = product.astype(jnp.float32)
    product = product - pulse_count * jnp.floor(product / pulse_count)
    phase = 2.0 * np.pi / pulse_count * product
    factor = 1.0 / np.sqrt(pulse_count)
    dop_r, dop_i = narrow(jnp.cos(phase) * factor), narrow(-jnp.sin(phase) * factor)
    count = channels * pulse_count
    factor = 1.0 / np.sqrt(count)
    t_r = t_i = None
    for band in range(bands):
        index = lax.broadcasted_iota(jnp.int32, (pulse_count, angles), 0) + band * pulse_count
        phase = (index.astype(jnp.float32) - 0.5 * count) * steer
        beam_r, beam_i = narrow(jnp.cos(phase) * factor), narrow(jnp.sin(phase) * factor)
        mixed = [[], []]
        for channel in range(channels):
            mix_r = mix_ref[0, band, channel : channel + 1, :]
            mix_i = mix_ref[1, band, channel : channel + 1, :]
            mixed[0].append(mix_r * dop_r - mix_i * dop_i)
            mixed[1].append(mix_r * dop_i + mix_i * dop_r)
        mixed_r, mixed_i = (jnp.concatenate(part, axis=0) for part in mixed)
        add_r = high_dot(mixed_r, beam_r) - high_dot(mixed_i, beam_i)
        add_i = high_dot(mixed_r, beam_i) + high_dot(mixed_i, beam_r)
        t_r = add_r if band == 0 else t_r + add_r
        t_i = add_i if band == 0 else t_i + add_i
    top = jnp.concatenate([t_r, t_i], axis=1)
    low = jnp.concatenate([-t_i, t_r], axis=1)
    return jnp.concatenate([top, low], axis=0)


def window_body(
    subs,
    filt_hbm,
    raw_hbm,
    mix_hbm,
    steer_hbm,
    offs_hbm,
    wts_hbm,
    rows_c,
    mix_ref,
    steer_ref,
    offs_ref,
    wts_ref,
    bsrc,
    ys,
    bg,
    echo,
    acc,
    base_hi,
    base_lo,
    fold_hi,
    fold_lo,
    ops,
    sbuf,
    img0,
    img_a,
    img_b,
    pbuf,
    loc_sem,
    y_s,
    y_r,
    bz_s,
    bz_r,
    bx_s,
    bx_r,
    a_s,
    a_r,
    sb_s,
    sb_r,
    sc_s,
    sc_r,
    h_s,
    h_r,
    up_sem,
    down_sem,
):
    chans = 2
    rows = bsrc.shape[1]
    half = ys.shape[2]
    pulses = echo.shape[3]
    own = img0.shape[2]
    angles = steer_ref.shape[1]
    feats = 2 * chans * pulses
    depth = subs // 4
    group = subs // 4
    levels = offs_ref.shape[0]

    s, c = lax.axis_index("sub"), lax.axis_index("chan")
    z, x, k = s // 4, (s // 2) % 2, s % 2
    par, zp = z % 2, z // 2

    def sub_at(dz, dx, dk):
        return flip(z, dz) * 4 + flip(x, dx) * 2 + flip(k, dk)

    def device(dz, dx, dk, dc):
        return {"sub": sub_at(dz, dx, dk), "chan": flip(c, dc)}

    def remote(src, dst, send, recv, dev):
        return pltpu.make_async_remote_copy(
            src_ref=src, dst_ref=dst, send_sem=send, recv_sem=recv, device_id=dev, device_id_type=MESH
        )

    q_me = par * 2 + k
    load_b = pltpu.make_async_copy(filt_hbm, bsrc, loc_sem.at[0])
    load_a = pltpu.make_async_copy(raw_hbm, echo.at[q_me, :, c], loc_sem.at[1])
    tables = [
        pltpu.make_async_copy(src, dst, loc_sem.at[2 + i])
        for i, (src, dst) in enumerate(
            [(offs_hbm, offs_ref), (wts_hbm, wts_ref), (mix_hbm, mix_ref), (steer_hbm, steer_ref)]
        )
    ]
    load_b.start()
    load_a.start()
    for table in tables:
        table.start()

    barrier = pltpu.get_barrier_semaphore()

    def greet(sub, chan):
        pl.semaphore_signal(barrier, inc=1, device_id={"sub": sub, "chan": chan}, device_id_type=MESH)

    def along(step, dk):
        return (z + step) * 4 + x * 2 + flip(k, dk)

    greet(s, 1 - c)
    greet(sub_at(0, 1, 0), c)
    greet(sub_at(0, 0, 1), c)
    below, above = z > 0, z < depth - 1

    @pl.when(below)
    def _():
        greet(along(-1, 0), c)
        greet(along(-1, 1), c)

    @pl.when(above)
    def _():
        greet(along(1, 0), c)
        greet(along(1, 1), c)

    pl.semaphore_wait(barrier, 3 + 2 * lax.min(z, 1) + 2 * lax.min(depth - 1 - z, 1))

    def tell(step, far, sem):
        pl.semaphore_signal(sem, inc=1, device_id={"sub": along(step, 0), "chan": c}, device_id_type=MESH)

    def spread_word(far):
        @pl.when(jnp.logical_and(below, z + far - 1 < depth))
        def _():
            tell(-1, far, up_sem.at[far - 2])

        @pl.when(jnp.logical_and(above, z - far + 1 >= 0))
        def _():
            tell(1, far, down_sem.at[far - 2])

        @pl.when(z + far < depth)
        def _():
            pl.semaphore_wait(up_sem.at[far - 2], 1)

        @pl.when(z - far >= 0)
        def _():
            pl.semaphore_wait(down_sem.at[far - 2], 1)

    sent = []

    def go(copy):
        copy.start()
        sent.append(copy)

    inner = (z + zp) % 2

    def reach(turn):
        if turn == 0:
            return z, 0
        if turn == 1:
            return flip(z, 1), 1
        if turn == 2:
            return depth // 2 - zp, 2 + inner
        return (depth - 1) * (1 - zp), 3 - inner

    def spot(at_z, dx, dk, dc):
        at = ((at_z * 4 + flip(x, dx) * 2 + flip(k, dk)) * chans + flip(c, dc)) * rows
        return bg.at[:, pl.ds(pl.multiple_of(at, rows), rows), :]

    def piece(at_z, dk, dc):
        column = ((at_z % 2) * 2 + flip(k, dk)) * LANES
        if dc:
            return ys.at[:, :, pl.ds(pl.multiple_of(column, LANES), LANES)]
        return bsrc.at[:, :, pl.ds(pl.multiple_of(c * half + column, LANES), LANES)]

    def block(turn, dk, dc):
        at_z, bits = reach(turn)
        to = {"sub": at_z * 4 + x * 2 + flip(k, dk), "chan": c}
        return remote(piece(at_z, dk, dc), spot(z, 0, 0, dc), bz_s.at[turn, dk, dc], bz_r.at[bits, dk, dc], to)

    def keep(dc):
        copy = pltpu.make_async_copy(piece(z, 0, dc), spot(z, 0, 0, dc), bz_r.at[0, 0, dc])
        copy.start()
        return copy

    def arrived(turn, dk, dc):
        at_z, bits = reach(turn)
        here = spot(at_z, 0, dk, dc)
        remote(here, here, bz_s.at[turn, dk, dc], bz_r.at[bits, dk, dc], device(0, 1, 0, 0)).wait_recv()

    def across(turn, dk, dc):
        at_z, bits = reach(turn)
        here = spot(at_z, 0, dk, dc)
        return remote(here, here, bx_s.at[turn, dk, dc], bx_r.at[bits, dk, dc], device(0, 1, 0, 0))

    def crossed(turn, dk, dc):
        at_z, bits = reach(turn)
        there = spot(at_z, 1, dk, dc)
        remote(there, there, bx_s.at[turn, dk, dc], bx_r.at[bits, dk, dc], device(0, 1, 0, 0)).wait_recv()

    def echo_at(da, dk, dc, part):
        return echo.at[flip(par, da) * 2 + flip(k, dk), part, flip(c, dc)]

    def pass_echo(slot, here, there, dev, part):
        spot_here = echo_at(*here, part)
        go(remote(spot_here, spot_here, a_s.at[slot, part], a_r.at[there + (part,)], device(*dev)))

    def echo_in(da, dk, dc, part):
        there = echo_at(da, dk, dc, part)
        remote(there, there, a_s.at[0, part], a_r.at[da, dk, dc, part], device(0, 0, 0, 1)).wait_recv()

    def build(level, side):
        block_rows = 32
        lane = side * angles
        offs = offs_ref[level : level + 1, lane : lane + angles]

        def strip(i, carry):
            at = pl.multiple_of(i * block_rows, block_rows)
            delta = lax.broadcasted_iota(jnp.int32, (block_rows, angles), 0) + at - offs
            band = [[jnp.zeros((block_rows, angles), jnp.float32)] * 2 for _ in range(2)]
            for j in range(wts_ref.shape[3]):
                hit = delta == j
                for child in range(2):
                    for part in range(2):
                        row = wts_ref[level, child, part, j : j + 1, lane : lane + angles]
                        band[child][part] = jnp.where(hit, row, band[child][part])
            left = 2 * lane
            for child in range(2):
                real, imag = band[child]
                for order in range(2 if level == 0 else 1):
                    r, m = real.astype(LOW), imag.astype(LOW)
                    if level == 0:
                        ref = (base_hi if order == 0 else base_lo).at[child]
                    else:
                        ref = ops.at[level - 1, child]
                    low = pl.ds(pl.multiple_of(angles + at, block_rows), block_rows)
                    ref[pl.ds(at, block_rows), left : left + angles] = r
                    ref[pl.ds(at, block_rows), left + angles : left + 2 * angles] = m
                    ref[low, left : left + angles] = -m
                    ref[low, left + angles : left + 2 * angles] = r
                    real, imag = real - r.astype(jnp.float32), imag - m.astype(jnp.float32)
            return carry

        lax.fori_loop(0, angles // block_rows, strip, 0)

    def fold():
        form = forming_rows(mix_ref, steer_ref[...], pulses)
        top = form.astype(LOW)
        low = (form - top.astype(jnp.float32)).astype(LOW)
        for child in range(2):
            hi, lo = base_hi[child], base_lo[child]
            value = low_dot(top, hi) + (low_dot(low, hi) + low_dot(top, lo))
            first = value.astype(LOW)
            at = slice(child * feats, (child + 1) * feats)
            fold_hi[at, :] = first
            fold_lo[at, :] = (value - first.astype(jnp.float32)).astype(LOW)

    def multiply(turn, dx, fresh):
        pair = reach(turn)[0] * 2 + flip(x, dx)
        wide = 2 * chans * rows
        at = pl.multiple_of(pair * wide, wide)
        left = echo[:, :, :, :, pl.ds(at, wide)].reshape(-1, wide)
        right = jnp.concatenate([bg[0, pl.ds(at, wide), :], bg[1, pl.ds(at, wide), :]], axis=1)
        value = low_dot(left, right)
        acc[...] = value if fresh else acc[...] + value

    other = pl.multiple_of((1 - c) * half, half)
    load_b.wait()
    go(remote(bsrc.at[:, :, pl.ds(other, half)], ys, y_s, y_r, device(0, 0, 0, 1)))
    kept = keep(0)
    go(block(0, 1, 0))
    load_a.wait()
    pass_echo(0, (0, 0, 0), (1, 0, 0), (1, 0, 0, 0), 0)
    pass_echo(1, (0, 0, 0), (0, 0, 1), (0, 0, 0, 1), 0)
    pass_echo(1, (0, 0, 0), (0, 0, 1), (0, 0, 0, 1), 1)
    for dk in range(2):
        go(block(1, dk, 0))
    pass_echo(2, (0, 0, 0), (0, 1, 0), (0, 0, 1, 0), 0)
    pass_echo(2, (0, 0, 0), (0, 1, 0), (0, 0, 1, 0), 1)
    far_pairs = [block(turn, dk, 0) for turn in range(2, depth) for dk in range(2)]
    sent.extend(far_pairs)

    @pl.when(inner == 1)
    def _():
        for copy in far_pairs[:2]:
            copy.start()

    kept.wait()
    go(across(0, 0, 0))
    spread_word(2)

    @pl.when(inner == 1)
    def _():
        for copy in far_pairs[2:]:
            copy.start()

    @pl.when(inner == 0)
    def _():
        for copy in far_pairs[:2]:
            copy.start()

    arrived(0, 1, 0)
    go(across(0, 1, 0))
    spread_word(3)

    @pl.when(inner == 0)
    def _():
        for copy in far_pairs[2:]:
            copy.start()

    pass_echo(0, (0, 0, 0), (1, 0, 0), (1, 0, 0, 0), 1)
    remote(ys, ys, y_s, y_r, device(0, 0, 0, 1)).wait_recv()
    kept = keep(1)
    go(block(0, 1, 1))
    go(block(1, 0, 1))
    go(block(1, 1, 1))
    go(block(2, 0, 1))
    go(block(2, 1, 1))
    go(block(3, 0, 1))
    go(block(3, 1, 1))
    kept.wait()
    go(across(0, 0, 1))
    for table in tables:
        table.wait()
    pending = [(level, side) for level in range(levels) for side in range(2)]
    build(*pending.pop(0))

    def relay(part):
        echo_in(1, 0, 0, part)
        pass_echo(3, (1, 0, 0), (1, 0, 1), (0, 0, 0, 1), part)
        pass_echo(4, (1, 0, 0), (1, 1, 0), (0, 0, 1, 0), part)

    def relay_side():
        for part in range(2):
            echo_in(0, 0, 1, part)
            pass_echo(5, (0, 0, 1), (0, 1, 1), (0, 0, 1, 0), part)

    relay(0)
    arrived(0, 1, 1)
    go(across(0, 1, 1))
    arrived(1, 0, 0)
    go(across(1, 0, 0))
    arrived(2, 0, 0)
    go(across(2, 0, 0))
    arrived(3, 0, 0)
    go(across(3, 0, 0))
    build(*pending.pop(0))
    arrived(1, 1, 0)
    go(across(1, 1, 0))
    arrived(2, 1, 0)
    go(across(2, 1, 0))
    arrived(3, 1, 0)
    go(across(3, 1, 0))
    build(*pending.pop(0))
    fold()
    relay(1)
    arrived(1, 0, 1)
    go(across(1, 0, 1))
    arrived(1, 1, 1)
    go(across(1, 1, 1))
    arrived(2, 0, 1)
    go(across(2, 0, 1))
    build(*pending.pop(0))
    relay_side()
    arrived(2, 1, 1)
    go(across(2, 1, 1))
    arrived(3, 0, 1)
    go(across(3, 0, 1))
    arrived(3, 1, 1)
    go(across(3, 1, 1))
    build(*pending.pop(0))
    for part in range(2):
        echo_in(1, 0, 1, part)
        pass_echo(6, (1, 0, 1), (1, 1, 1), (0, 0, 1, 0), part)
    while pending:
        build(*pending.pop(0))
    for da in range(2):
        for dc in range(2):
            for part in range(2):
                echo_in(da, 1, dc, part)
    multiply(0, 0, True)
    for turn in range(1, depth):
        multiply(turn, 0, False)
    for turn in range(depth):
        for dk in range(2):
            for dc in range(2):
                crossed(turn, dk, dc)
        multiply(turn, 1, False)

    value = acc[...].reshape(4, 2, feats // 2, 2 * LANES)
    for q in range(4):
        real = value[q, 0, :, :LANES] - value[q, 1, :, LANES:]
        imag = value[q, 0, :, LANES:] + value[q, 1, :, :LANES]
        turned = jnp.concatenate([real, imag], axis=0).T.astype(LOW)
        sbuf[:, q] = turned.reshape(group, own, feats)
    mine = zp * 2 + x
    spread = [(dzp, dx) for dzp in range(depth // 2 - 1, -1, -1) for dx in (1, 0)]
    for dzp, dx in spread:
        slot = dzp * 2 + dx
        if slot:
            to = flip(zp, dzp) * 2 + flip(x, dx)
            go(remote(sbuf.at[to], img0.at[mine], sb_s.at[slot], sb_r.at[slot], device(2 * dzp, dx, 0, 0)))
    img0[mine] = sbuf[mine]
    while len(sent) > group - 1:
        sent.pop(0).wait_send()
    for dzp, dx in spread:
        slot = dzp * 2 + dx
        if slot:
            origin = flip(zp, dzp) * 2 + flip(x, dx)
            remote(
                sbuf.at[origin], img0.at[origin], sb_s.at[slot], sb_r.at[slot], device(2 * dzp, dx, 0, 0)
            ).wait_recv()

    place = (depth // 2, 2, 2, 2)
    wide = 2 * angles

    def child_rows(ref, axis, child, cols):
        split = (place[0] // 2, 2) + place[1:] if axis == 0 else place
        at = 1 if axis == 0 else axis
        whole = ref[...].reshape(split + (own, cols))
        return lax.index_in_dim(whole, child, at, keepdims=False).reshape(-1, cols)

    axis_of = [3, 1, 2] + [0] * (levels - 3)
    pair = jnp.concatenate([child_rows(img0, 3, child, feats) for child in range(2)], axis=1)
    source, target = img_a, img_b
    for side in range(2):
        cols = slice(side * wide, (side + 1) * wide)
        out = low_dot(pair, fold_hi[:, cols]) + low_dot(pair, fold_lo[:, cols])
        source[:, :, :, side] = out.astype(LOW).reshape(place[:3] + (own, wide))
    for level in range(1, levels - 1):
        first, second = (child_rows(source, axis_of[level], child, wide) for child in range(2))
        for side in range(2):
            cols = slice(side * wide, (side + 1) * wide)
            out = low_dot(first, ops[level - 1, 0, :, cols]) + low_dot(second, ops[level - 1, 1, :, cols])
            out = out.astype(LOW)
            if axis_of[level] == 1:
                target[:, side] = out.reshape(place[0], 2, 2, own, wide)
            else:
                target[:, :, side] = out.reshape(place[0], 2, 2, own, wide)
        source, target = target, source
    first, second = (child_rows(source, 0, child, wide) for child in range(2))
    base = HALO + (q_me * group + mine) * own
    block_at = pl.multiple_of(base, HALO)

    for turn in (1, 0):
        side = flip(zp, turn) % 2
        cols = pl.ds(pl.multiple_of(side * wide, wide), wide)
        out = low_dot(first, ops[levels - 2, 0, :, cols]) + low_dot(second, ops[levels - 2, 1, :, cols])
        power = out[:, :angles] * out[:, :angles] + out[:, angles:] * out[:, angles:]
        power = power.astype(LOW).reshape(place[0] // 2, 2, 2, 2, own, angles)
        for pair_at in range(place[0] // 2):
            pbuf[pair_at * 2 + side] = power[pair_at]
        for high in range(place[0] // 2):
            dzp = high * 2 + turn
            for rel in range(8):
                dx, dzz, dk = rel // 4, (rel // 2) % 2, rel % 2
                slot = dzp * 8 + rel
                src = pbuf.at[flip(zp, dzp), flip(x, dx), flip(par, dzz), flip(k, dk)]
                if slot:
                    go(
                        remote(
                            src,
                            rows_c.at[pl.ds(block_at, own), :],
                            sc_s.at[slot],
                            sc_r.at[slot],
                            device(2 * dzp + dzz, dx, dk, 0),
                        )
                    )

    rows_c[pl.ds(block_at, own), :] = pbuf[zp, x, par, k]

    @pl.when(c == 0)
    def _():
        rows_c[pl.ds(0, HALO), :] = jnp.zeros((HALO, angles), LOW)

    @pl.when(c == 1)
    def _():
        rows_c[pl.ds(HALO + half, HALO), :] = jnp.zeros((HALO, angles), LOW)

    def landed(slot):
        dzp, rel = slot // 8, slot % 8
        at_zp, at_x = across_bit(zp, dzp), across_bit(x, rel // 4)
        at_par, at_k = across_bit(par, (rel // 2) % 2), across_bit(k, rel % 2)
        at = HALO + ((at_par * 2 + at_k) * group + at_zp * 2 + at_x) * own
        dst = rows_c.at[pl.ds(pl.multiple_of(at, HALO), own), :]
        remote(dst, dst, sc_s.at[slot], sc_r.at[slot], device(0, 0, 0, 1)).wait_recv()

    def across_bit(bit, change):
        return bit + change - 2 * bit * change

    here = ((zp * 2 + x) * 2 + par) * 2 + k
    edge = here * c + (subs - 1 - here) * (1 - c)

    @pl.when(edge != 0)
    def _():
        landed(edge)

    border = remote(
        rows_c.at[pl.ds(pl.multiple_of(half * (1 - c) + HALO * c, HALO), HALO), :],
        rows_c.at[pl.ds(pl.multiple_of((HALO + half) * c, HALO), HALO), :],
        h_s,
        h_r,
        device(0, 0, 0, 1),
    )
    border.start()
    for slot in range(subs - 1, 0, -1):

        @pl.when(edge != slot)
        def _():
            landed(slot)

    far_border = rows_c.at[pl.ds(pl.multiple_of((HALO + half) * (1 - c), HALO), HALO), :]
    remote(far_border, far_border, h_s, h_r, device(0, 0, 0, 1)).wait_recv()
    border.wait_send()
    for copy in sent:
        copy.wait_send()


def smooth_body(chans, power_ref, rate_ref, out_hbm, turned, sem):
    at = lax.axis_index("chan")
    height = turned.shape[1]
    shape = (height + 2 * HALO, LANES)
    row = lax.broadcasted_iota(jnp.int32, shape, 0)
    inside = jnp.logical_and(
        jnp.logical_or(row >= HALO, at > 0), jnp.logical_or(row < HALO + height, at < chans - 1)
    )
    copies = []
    for part in range(turned.shape[0] // LANES):
        cols = slice(part * LANES, (part + 1) * LANES)
        power = power_ref[:, cols].astype(jnp.float32)
        rate = rate_ref[:, cols]
        for sweep in range(PASSES):
            before = pltpu.roll(power, 1, 0)
            after = pltpu.roll(power, shape[0] - 1, 0)
            power = power + rate * (before - 2.0 * power + after)
            power = jnp.where(inside, power, 0.0)
        turned[cols, :] = power[HALO : HALO + height].T
        copy = pltpu.make_async_copy(turned.at[cols, :], out_hbm.at[cols, :], sem.at[part])
        copy.start()
        copies.append(copy)
    for copy in copies:
        copy.wait()


def local_kernel(
    raw_pulses, range_filter, channel_mix, steer_angles, band_offsets, band_weights, smoothing
):
    _, pulses, _, samples = raw_pulses.shape
    _, rows, bins = range_filter.shape
    angles = steer_angles.shape[0]
    levels, _, _, merged, band_width = band_weights.shape
    subs, chans = lax.axis_size("sub"), lax.axis_size("chan")
    half = bins // chans
    group = subs // 4
    own = LANES // group
    depth = subs // 4
    feats = 2 * chans * pulses
    place = (depth // 2, 2, 2, 2)
    dma = pltpu.SemaphoreType.DMA
    vmem = pl.BlockSpec(memory_space=pltpu.VMEM)
    anywhere = pl.BlockSpec(memory_space=pl.ANY)
    power = pl.pallas_call(
        functools.partial(window_body, subs),
        out_shape=jax.ShapeDtypeStruct((half + 2 * HALO, angles), LOW),
        in_specs=[pl.BlockSpec(memory_space=pltpu.HBM)] * 6,
        out_specs=vmem,
        scratch_shapes=[
            pltpu.VMEM((2, chans, chans, pulses), jnp.float32),
            pltpu.VMEM((1, angles), jnp.float32),
            pltpu.VMEM((levels, merged), jnp.int32),
            pltpu.VMEM((levels, 2, 2, band_width, merged), jnp.float32),
            pltpu.VMEM((2, rows, bins), LOW),
            pltpu.VMEM((2, rows, half), LOW),
            pltpu.VMEM((2, subs * chans * rows, LANES), LOW),
            pltpu.VMEM((4, 2, chans, pulses, samples), LOW),
            pltpu.VMEM((4 * feats, 2 * LANES), jnp.float32),
            pltpu.VMEM((2, 2 * angles, 2 * merged), LOW),
            pltpu.VMEM((2, 2 * angles, 2 * merged), LOW),
            pltpu.VMEM((2 * feats, 2 * merged), LOW),
            pltpu.VMEM((2 * feats, 2 * merged), LOW),
            pltpu.VMEM((levels - 1, 2, 2 * angles, 2 * merged), LOW),
            pltpu.VMEM((group, 4, own, feats), LOW),
            pltpu.VMEM((group, 4, own, feats), LOW),
            pltpu.VMEM(place + (own, 2 * angles), LOW),
            pltpu.VMEM(place + (own, 2 * angles), LOW),
            pltpu.VMEM(place + (own, angles), LOW),
            dma((6,)),
            dma,
            dma,
            dma((depth, 2, 2)),
            dma((depth, 2, 2)),
            dma((depth, 2, 2)),
            dma((depth, 2, 2)),
            dma((7, 2)),
            dma((2, 2, 2, 2)),
            dma((group,)),
            dma((group,)),
            dma((subs,)),
            dma((subs,)),
            dma,
            dma,
            pltpu.SemaphoreType.REGULAR((depth - 2,)),
            pltpu.SemaphoreType.REGULAR((depth - 2,)),
        ],
        compiler_params=pltpu.CompilerParams(
            collective_id=0, has_side_effects=True, vmem_limit_bytes=32 << 20
        ),
    )(
        *(
            pltpu.with_memory_space_constraint(array, pltpu.HBM)
            for array in (
                range_filter,
                raw_pulses[:, :, 0, :],
                channel_mix.transpose(0, 2, 3, 1),
                steer_angles[None, :],
                band_offsets,
                band_weights.transpose(0, 1, 2, 4, 3),
            )
        )
    )
    return pl.pallas_call(
        functools.partial(smooth_body, chans),
        out_shape=jax.ShapeDtypeStruct((angles, half), jnp.float32),
        in_specs=[vmem, vmem],
        out_specs=anywhere,
        scratch_shapes=[pltpu.VMEM((angles, half), jnp.float32), dma((angles // LANES,))],
        compiler_params=pltpu.CompilerParams(vmem_limit_bytes=8 << 20),
    )(power, smoothing[None, :])


def fits(mesh, raw_pulses, range_filter, steer_angles, band_offsets):
    subs, chans = mesh.shape["sub"], mesh.shape["chan"]
    rows = range_filter.shape[1] // (subs * chans)
    pulses = raw_pulses.shape[1] // subs
    cut = chans == 2 and subs // 4 == 4
    cut = cut and range_filter.shape[2] == 4 * chans * LANES and LANES // (subs // 4) >= HALO
    cut = cut and rows % 16 == 0 and pulses % 16 == 0 and steer_angles.shape[0] % LANES == 0
    return cut and band_offsets.shape[0] == 4


def solution(mesh):
    in_specs = (
        P(None, "sub", "chan", None),
        P(None, ("sub", "chan"), None),
        P(),
        P(),
        P(),
        P(),
        P("sub"),
    )
    out_specs = P("sub", "chan")

    def run(raw_pulses, range_filter, channel_mix, steer_angles, band_offsets, band_weights, smoothing):
        one = local_kernel if fits(mesh, raw_pulses, range_filter, steer_angles, band_offsets) else local_plain
        part = jax.shard_map(one, mesh=mesh, in_specs=in_specs, out_specs=out_specs, check_vma=False)
        return part(
            raw_pulses, range_filter, channel_mix, steer_angles, band_offsets, band_weights, smoothing
        )

    return run
```

```python
import functools

import jax
import jax.numpy as jnp
import numpy as np
from jax import lax
from jax.experimental import pallas as pl
from jax.experimental.pallas import tpu as pltpu
from jax.sharding import PartitionSpec as P

PASSES = 3
HALO = 16
LANES = 128
HIGH = lax.Precision.HIGHEST
LOW = jnp.bfloat16
MESH = pl.DeviceIdType.MESH
def rounded(value):
    return lax.reduce_precision(value, exponent_bits=8, mantissa_bits=7)


def halves(value):
    top = rounded(value)
    return top.astype(LOW), (value - top).astype(LOW)


def doppler_table(count):
    index_row = jnp.arange(count, dtype=jnp.int32)
    product = index_row[:, None] * index_row[None, :] % count
    phase = 2.0 * np.pi / count * product.astype(jnp.float32)
    factor = 1.0 / np.sqrt(count)
    return (
        rounded(jnp.cos(phase) * factor),
        rounded(-jnp.sin(phase) * factor),
    )


def steer_table(steer_angles, count):
    offsets = jnp.arange(count, dtype=jnp.int32).astype(jnp.float32) - 0.5 * count
    phase = offsets[:, None] * steer_angles[None, :]
    factor = 1.0 / np.sqrt(count)
    return (
        rounded(jnp.cos(phase) * factor),
        rounded(jnp.sin(phase) * factor),
    )


def forming_operator(channel_mix, steer_angles, pulse_count):
    channels = channel_mix.shape[2]
    dop_r, dop_i = doppler_table(pulse_count)
    beam_r, beam_i = steer_table(steer_angles, channels * pulse_count)
    mix = channel_mix.transpose(0, 3, 2, 1)[:, :, None, :, :]
    dr, di = dop_r.T[None, :, None, :], dop_i.T[None, :, None, :]
    shape = (channels * pulse_count, channels * pulse_count)
    mixed_r = (mix[0] * dr - mix[1] * di).reshape(shape)
    mixed_i = (mix[0] * di + mix[1] * dr).reshape(shape)
    left = jnp.concatenate([mixed_r, mixed_i], axis=1)
    t_r = jnp.dot(left, jnp.concatenate([beam_r, -beam_i], axis=0), precision=HIGH)
    t_i = jnp.dot(left, jnp.concatenate([beam_i, beam_r], axis=0), precision=HIGH)
    angles = steer_angles.shape[0]
    t_r = t_r.reshape(channels, pulse_count, angles)
    t_i = t_i.reshape(channels, pulse_count, angles)
    top = jnp.concatenate([t_r, t_i], axis=2)
    low = jnp.concatenate([-t_i, t_r], axis=2)
    both = jnp.concatenate([top, low], axis=1)
    return both.reshape(channels * 2 * pulse_count, 2 * angles)


def operator_body(offsets_ref, weights_ref, *out_refs):
    band_width, count = weights_ref.shape[3], weights_ref.shape[4]
    delta = lax.broadcasted_iota(jnp.int32, (count, count), 0) - offsets_ref[0]
    bands = [jnp.zeros((count, count), jnp.float32)] * 2
    for j in range(band_width):
        hit = delta == j
        bands = [
            jnp.where(hit, weights_ref[0, 0, part, j : j + 1, :], bands[part]) for part in range(2)
        ]
    for order, ref in enumerate(out_refs):
        real, imag = (band.astype(LOW) for band in bands)
        ref[0, 0, :count, :count] = real
        ref[0, 0, :count, count:] = imag
        ref[0, 0, count:, :count] = -imag
        ref[0, 0, count:, count:] = real
        if order + 1 < len(out_refs):
            bands = [band - band.astype(LOW).astype(jnp.float32) for band in bands]


def merge_operators(offsets, weights, parts):
    levels, _, _, merged, band_width = weights.shape
    count = merged // 2
    by_step = weights.transpose(0, 1, 2, 4, 3)
    shape = jax.ShapeDtypeStruct((levels, 2, 2 * count, 2 * merged), LOW)
    return pl.pallas_call(
        operator_body,
        grid=(levels, 2, 2),
        in_specs=[
            pl.BlockSpec((1, 1, count), lambda l, c, h: (l, 0, h)),
            pl.BlockSpec((1, 1, 2, band_width, count), lambda l, c, h: (l, c, 0, 0, h)),
        ],
        out_specs=[
            pl.BlockSpec((1, 1, 2 * count, 2 * count), lambda l, c, h: (l, c, 0, h))
        ] * parts,
        out_shape=[shape] * parts,
        cost_estimate=pl.CostEstimate(
            flops=levels * 4 * count * count * 32,
            bytes_accessed=levels * parts * 16 * count * count * 2,
            transcendentals=0,
        ),
    )(offsets[:, None, :], by_step)


def low_dot(left, right):
    return jnp.dot(left, right, preferred_element_type=jnp.float32)


def local_plain(
    raw_pulses, range_filter, channel_mix, steer_angles, band_offsets, band_weights, smoothing
):
    pulses = raw_pulses.shape[1]
    samples = raw_pulses.shape[3]
    bins = range_filter.shape[2]
    angles = steer_angles.shape[0]
    levels = band_offsets.shape[0]
    subs, chans = lax.axis_size("sub"), lax.axis_size("chan")
    own = bins // (subs * chans)

    part = lax.all_to_all(range_filter, "chan", split_axis=2, concat_axis=1, tiled=True)
    filt = lax.all_gather(part, "sub", axis=1, tiled=True)
    echo = lax.all_gather(raw_pulses[:, :, 0, :], "chan", axis=0)

    forming = forming_operator(channel_mix, steer_angles, pulses)
    form_top, form_low = halves(forming)
    base_top, base_low = merge_operators(band_offsets[:1], band_weights[:1], 2)
    folded = [
        low_dot(form_top, base_top[0, c])
        + (low_dot(form_low, base_top[0, c]) + low_dot(form_top, base_low[0, c]))
        for c in range(2)
    ]
    folded_top, folded_low = halves(jnp.concatenate(folded, axis=0))
    (later,) = merge_operators(band_offsets[1:], band_weights[1:], 1)

    real_rows = jnp.concatenate([echo[:, 0], -echo[:, 1]], axis=2)
    imag_rows = jnp.concatenate([echo[:, 1], echo[:, 0]], axis=2)
    stacked = jnp.concatenate([real_rows, imag_rows], axis=1).reshape(-1, 2 * samples)
    compressed = low_dot(stacked, filt.reshape(2 * samples, -1)).astype(LOW)
    blocks = compressed.T.reshape(subs, own, -1)
    got = lax.all_to_all(blocks, "sub", split_axis=0, concat_axis=0, tiled=True)
    image = got.reshape(subs * own, -1)
    for level in range(levels):
        run = (1 << level) * own
        wide = image.shape[1]
        field = image.astype(LOW).reshape(-1, 2, run, wide)
        pair = jnp.concatenate([field[:, 0], field[:, 1]], axis=2).reshape(-1, 2 * wide)
        if level == 0:
            out = low_dot(pair, folded_top) + low_dot(pair, folded_low)
        else:
            out = low_dot(pair, later[level - 1].reshape(2 * wide, -1))
        out = out.reshape(-1, run, 4 * angles)
        image = jnp.stack([out[:, :, : 2 * angles], out[:, :, 2 * angles :]], axis=1)
        image = image.reshape(-1, 2 * angles)
    power = image[:, :angles] * image[:, :angles] + image[:, angles:] * image[:, angles:]
    power = power.astype(LOW).reshape(subs, own, angles)
    power = lax.all_to_all(power, "sub", split_axis=0, concat_axis=0, tiled=True)
    power = power.reshape(subs * own, angles)
    up = [(i, i + 1) for i in range(chans - 1)]
    down = [(j, i) for i, j in up]
    before = lax.ppermute(power[-PASSES:], "chan", up).astype(jnp.float32)
    after = lax.ppermute(power[:PASSES], "chan", down).astype(jnp.float32)
    power = jnp.concatenate([before, power.astype(jnp.float32), after], axis=0)
    rate = smoothing[None, :]
    at = lax.axis_index("chan")
    lead, trail = at == 0, at == chans - 1
    for sweep in range(PASSES):
        mid = power[1:-1]
        power = mid + rate * (power[:-2] - 2.0 * mid + power[2:])
        edge = PASSES - 1 - sweep
        if edge:
            inner = power[edge:-edge]
            head = jnp.where(lead, 0.0, power[:edge])
            tail = jnp.where(trail, 0.0, power[-edge:])
            power = jnp.concatenate([head, inner, tail], axis=0)
    return power.T


def narrow(value):
    return value.astype(LOW).astype(jnp.float32)


def high_dot(left, right):
    return jnp.dot(left, right, precision=HIGH, preferred_element_type=jnp.float32)


def flip(value, bits):
    out = value
    step = 1
    while step <= bits:
        if bits & step:
            out = out + step - 2 * step * ((value // step) % 2)
        step *= 2
    return out


def forming_rows(mix_ref, steer, pulse_count):
    bands, channels = mix_ref.shape[1], mix_ref.shape[2]
    angles = steer.shape[1]
    square = (pulse_count, pulse_count)
    product = lax.broadcasted_iota(jnp.int32, square, 0) * lax.broadcasted_iota(jnp.int32, square, 1)
    product = product.astype(jnp.float32)
    product = product - pulse_count * jnp.floor(product / pulse_count)
    phase = 2.0 * np.pi / pulse_count * product
    factor = 1.0 / np.sqrt(pulse_count)
    dop_r, dop_i = narrow(jnp.cos(phase) * factor), narrow(-jnp.sin(phase) * factor)
    count = channels * pulse_count
    factor = 1.0 / np.sqrt(count)
    t_r = t_i = None
    for band in range(bands):
        index = lax.broadcasted_iota(jnp.int32, (pulse_count, angles), 0) + band * pulse_count
        phase = (index.astype(jnp.float32) - 0.5 * count) * steer
        beam_r, beam_i = narrow(jnp.cos(phase) * factor), narrow(jnp.sin(phase) * factor)
        mixed = [[], []]
        for channel in range(channels):
            mix_r = mix_ref[0, band, channel : channel + 1, :]
            mix_i = mix_ref[1, band, channel : channel + 1, :]
            mixed[0].append(mix_r * dop_r - mix_i * dop_i)
            mixed[1].append(mix_r * dop_i + mix_i * dop_r)
        mixed_r, mixed_i = (jnp.concatenate(part, axis=0) for part in mixed)
        add_r = high_dot(mixed_r, beam_r) - high_dot(mixed_i, beam_i)
        add_i = high_dot(mixed_r, beam_i) + high_dot(mixed_i, beam_r)
        t_r = add_r if band == 0 else t_r + add_r
        t_i = add_i if band == 0 else t_i + add_i
    top = jnp.concatenate([t_r, t_i], axis=1)
    low = jnp.concatenate([-t_i, t_r], axis=1)
    return jnp.concatenate([top, low], axis=0)


def window_body(
    subs,
    filt_hbm,
    raw_hbm,
    mix_hbm,
    steer_hbm,
    offs_hbm,
    wts_hbm,
    rows_c,
    mix_ref,
    steer_ref,
    offs_ref,
    wts_ref,
    bsrc,
    ys,
    bg,
    echo,
    acc,
    base_hi,
    base_lo,
    fold_hi,
    fold_lo,
    ops,
    sbuf,
    img0,
    img_a,
    img_b,
    pbuf,
    loc_sem,
    y_s,
    y_r,
    bz_s,
    bz_r,
    bx_s,
    bx_r,
    a_s,
    a_r,
    sb_s,
    sb_r,
    sc_s,
    sc_r,
    h_s,
    h_r,
    up_sem,
    down_sem,
):
    chans = 2
    rows = bsrc.shape[1]
    half = ys.shape[2]
    pulses = echo.shape[3]
    own = img0.shape[2]
    angles = steer_ref.shape[1]
    feats = 2 * chans * pulses
    depth = subs // 4
    group = subs // 4
    levels = offs_ref.shape[0]

    s, c = lax.axis_index("sub"), lax.axis_index("chan")
    z, x, k = s // 4, (s // 2) % 2, s % 2
    par, zp = z % 2, z // 2

    def sub_at(dz, dx, dk):
        return flip(z, dz) * 4 + flip(x, dx) * 2 + flip(k, dk)

    def device(dz, dx, dk, dc):
        return {"sub": sub_at(dz, dx, dk), "chan": flip(c, dc)}

    def remote(src, dst, send, recv, dev):
        return pltpu.make_async_remote_copy(
            src_ref=src, dst_ref=dst, send_sem=send, recv_sem=recv, device_id=dev, device_id_type=MESH
        )

    q_me = par * 2 + k
    load_b = pltpu.make_async_copy(filt_hbm, bsrc, loc_sem.at[0])
    load_a = pltpu.make_async_copy(raw_hbm, echo.at[q_me, :, c], loc_sem.at[1])
    tables = [
        pltpu.make_async_copy(src, dst, loc_sem.at[2 + i])
        for i, (src, dst) in enumerate(
            [(offs_hbm, offs_ref), (wts_hbm, wts_ref), (mix_hbm, mix_ref), (steer_hbm, steer_ref)]
        )
    ]
    load_b.start()
    load_a.start()
    for table in tables:
        table.start()

    barrier = pltpu.get_barrier_semaphore()

    def greet(sub, chan):
        pl.semaphore_signal(barrier, inc=1, device_id={"sub": sub, "chan": chan}, device_id_type=MESH)

    def along(step, dk):
        return (z + step) * 4 + x * 2 + flip(k, dk)

    greet(s, 1 - c)
    greet(sub_at(0, 1, 0), c)
    greet(sub_at(0, 0, 1), c)
    below, above = z > 0, z < depth - 1

    @pl.when(below)
    def _():
        greet(along(-1, 0), c)
        greet(along(-1, 1), c)

    @pl.when(above)
    def _():
        greet(along(1, 0), c)
        greet(along(1, 1), c)

    pl.semaphore_wait(barrier, 3 + 2 * lax.min(z, 1) + 2 * lax.min(depth - 1 - z, 1))

    def tell(step, far, sem):
        pl.semaphore_signal(sem, inc=1, device_id={"sub": along(step, 0), "chan": c}, device_id_type=MESH)

    def spread_word(far):
        @pl.when(jnp.logical_and(below, z + far - 1 < depth))
        def _():
            tell(-1, far, up_sem.at[far - 2])

        @pl.when(jnp.logical_and(above, z - far + 1 >= 0))
        def _():
            tell(1, far, down_sem.at[far - 2])

        @pl.when(z + far < depth)
        def _():
            pl.semaphore_wait(up_sem.at[far - 2], 1)

        @pl.when(z - far >= 0)
        def _():
            pl.semaphore_wait(down_sem.at[far - 2], 1)

    sent = []

    def go(copy):
        copy.start()
        sent.append(copy)

    inner = (z + zp) % 2

    def reach(turn):
        if turn == 0:
            return z, 0
        if turn == 1:
            return flip(z, 1), 1
        if turn == 2:
            return depth // 2 - zp, 2 + inner
        return (depth - 1) * (1 - zp), 3 - inner

    def spot(at_z, dx, dk, dc):
        at = ((at_z * 4 + flip(x, dx) * 2 + flip(k, dk)) * chans + flip(c, dc)) * rows
        return bg.at[:, pl.ds(pl.multiple_of(at, rows), rows), :]

    def piece(at_z, dk, dc):
        column = ((at_z % 2) * 2 + flip(k, dk)) * LANES
        if dc:
            return ys.at[:, :, pl.ds(pl.multiple_of(column, LANES), LANES)]
        return bsrc.at[:, :, pl.ds(pl.multiple_of(c * half + column, LANES), LANES)]

    def block(turn, dk, dc):
        at_z, bits = reach(turn)
        to = {"sub": at_z * 4 + x * 2 + flip(k, dk), "chan": c}
        return remote(piece(at_z, dk, dc), spot(z, 0, 0, dc), bz_s.at[turn, dk, dc], bz_r.at[bits, dk, dc], to)

    def keep(dc):
        copy = pltpu.make_async_copy(piece(z, 0, dc), spot(z, 0, 0, dc), bz_r.at[0, 0, dc])
        copy.start()
        return copy

    def arrived(turn, dk, dc):
        at_z, bits = reach(turn)
        here = spot(at_z, 0, dk, dc)
        remote(here, here, bz_s.at[turn, dk, dc], bz_r.at[bits, dk, dc], device(0, 1, 0, 0)).wait_recv()

    def across(turn, dk, dc):
        at_z, bits = reach(turn)
        here = spot(at_z, 0, dk, dc)
        return remote(here, here, bx_s.at[turn, dk, dc], bx_r.at[bits, dk, dc], device(0, 1, 0, 0))

    def crossed(turn, dk, dc):
        at_z, bits = reach(turn)
        there = spot(at_z, 1, dk, dc)
        remote(there, there, bx_s.at[turn, dk, dc], bx_r.at[bits, dk, dc], device(0, 1, 0, 0)).wait_recv()

    def echo_at(da, dk, dc, part):
        return echo.at[flip(par, da) * 2 + flip(k, dk), part, flip(c, dc)]

    def pass_echo(slot, here, there, dev, part):
        spot_here = echo_at(*here, part)
        go(remote(spot_here, spot_here, a_s.at[slot, part], a_r.at[there + (part,)], device(*dev)))

    def echo_in(da, dk, dc, part):
        there = echo_at(da, dk, dc, part)
        remote(there, there, a_s.at[0, part], a_r.at[da, dk, dc, part], device(0, 0, 0, 1)).wait_recv()

    def build(level, side):
        block_rows = 32
        lane = side * angles
        offs = offs_ref[level : level + 1, lane : lane + angles]

        def strip(i, carry):
            at = pl.multiple_of(i * block_rows, block_rows)
            delta = lax.broadcasted_iota(jnp.int32, (block_rows, angles), 0) + at - offs
            band = [[jnp.zeros((block_rows, angles), jnp.float32)] * 2 for _ in range(2)]
            for j in range(wts_ref.shape[3]):
                hit = delta == j
                for child in range(2):
                    for part in range(2):
                        row = wts_ref[level, child, part, j : j + 1, lane : lane + angles]
                        band[child][part] = jnp.where(hit, row, band[child][part])
            left = 2 * lane
            for child in range(2):
                real, imag = band[child]
                for order in range(2 if level == 0 else 1):
                    r, m = real.astype(LOW), imag.astype(LOW)
                    if level == 0:
                        ref = (base_hi if order == 0 else base_lo).at[child]
                    else:
                        ref = ops.at[level - 1, child]
                    low = pl.ds(pl.multiple_of(angles + at, block_rows), block_rows)
                    ref[pl.ds(at, block_rows), left : left + angles] = r
                    ref[pl.ds(at, block_rows), left + angles : left + 2 * angles] = m
                    ref[low, left : left + angles] = -m
                    ref[low, left + angles : left + 2 * angles] = r
                    real, imag = real - r.astype(jnp.float32), imag - m.astype(jnp.float32)
            return carry

        lax.fori_loop(0, angles // block_rows, strip, 0)

    def fold():
        form = forming_rows(mix_ref, steer_ref[...], pulses)
        top = form.astype(LOW)
        low = (form - top.astype(jnp.float32)).astype(LOW)
        for child in range(2):
            hi, lo = base_hi[child], base_lo[child]
            value = low_dot(top, hi) + (low_dot(low, hi) + low_dot(top, lo))
            first = value.astype(LOW)
            at = slice(child * feats, (child + 1) * feats)
            fold_hi[at, :] = first
            fold_lo[at, :] = (value - first.astype(jnp.float32)).astype(LOW)

    def multiply(turn, dx, fresh):
        pair = reach(turn)[0] * 2 + flip(x, dx)
        wide = 2 * chans * rows
        at = pl.multiple_of(pair * wide, wide)
        left = echo[:, :, :, :, pl.ds(at, wide)].reshape(-1, wide)
        right = jnp.concatenate([bg[0, pl.ds(at, wide), :], bg[1, pl.ds(at, wide), :]], axis=1)
        value = low_dot(left, right)
        acc[...] = value if fresh else acc[...] + value

    other = pl.multiple_of((1 - c) * half, half)
    load_b.wait()
    go(remote(bsrc.at[:, :, pl.ds(other, half)], ys, y_s, y_r, device(0, 0, 0, 1)))
    kept = keep(0)
    go(block(0, 1, 0))
    load_a.wait()
    pass_echo(0, (0, 0, 0), (1, 0, 0), (1, 0, 0, 0), 0)
    pass_echo(1, (0, 0, 0), (0, 0, 1), (0, 0, 0, 1), 0)
    pass_echo(1, (0, 0, 0), (0, 0, 1), (0, 0, 0, 1), 1)
    for dk in range(2):
        go(block(1, dk, 0))
    pass_echo(2, (0, 0, 0), (0, 1, 0), (0, 0, 1, 0), 0)
    pass_echo(2, (0, 0, 0), (0, 1, 0), (0, 0, 1, 0), 1)
    far_pairs = [block(turn, dk, 0) for turn in range(2, depth) for dk in range(2)]
    sent.extend(far_pairs)

    @pl.when(inner == 1)
    def _():
        for copy in far_pairs[:2]:
            copy.start()

    kept.wait()
    go(across(0, 0, 0))
    spread_word(2)

    @pl.when(inner == 1)
    def _():
        for copy in far_pairs[2:]:
            copy.start()

    @pl.when(inner == 0)
    def _():
        for copy in far_pairs[:2]:
            copy.start()

    arrived(0, 1, 0)
    go(across(0, 1, 0))
    spread_word(3)

    @pl.when(inner == 0)
    def _():
        for copy in far_pairs[2:]:
            copy.start()

    pass_echo(0, (0, 0, 0), (1, 0, 0), (1, 0, 0, 0), 1)
    remote(ys, ys, y_s, y_r, device(0, 0, 0, 1)).wait_recv()
    kept = keep(1)
    go(block(0, 1, 1))
    go(block(1, 0, 1))
    go(block(1, 1, 1))
    go(block(2, 0, 1))
    go(block(2, 1, 1))
    go(block(3, 0, 1))
    go(block(3, 1, 1))
    kept.wait()
    go(across(0, 0, 1))
    for table in tables:
        table.wait()
    pending = [(level, side) for level in range(levels) for side in range(2)]
    build(*pending.pop(0))

    def relay(part):
        echo_in(1, 0, 0, part)
        pass_echo(3, (1, 0, 0), (1, 0, 1), (0, 0, 0, 1), part)
        pass_echo(4, (1, 0, 0), (1, 1, 0), (0, 0, 1, 0), part)

    def relay_side():
        for part in range(2):
            echo_in(0, 0, 1, part)
            pass_echo(5, (0, 0, 1), (0, 1, 1), (0, 0, 1, 0), part)

    relay(0)
    arrived(0, 1, 1)
    go(across(0, 1, 1))
    arrived(1, 0, 0)
    go(across(1, 0, 0))
    arrived(2, 0, 0)
    go(across(2, 0, 0))
    arrived(3, 0, 0)
    go(across(3, 0, 0))
    build(*pending.pop(0))
    arrived(1, 1, 0)
    go(across(1, 1, 0))
    arrived(2, 1, 0)
    go(across(2, 1, 0))
    arrived(3, 1, 0)
    go(across(3, 1, 0))
    build(*pending.pop(0))
    fold()
    relay(1)
    arrived(1, 0, 1)
    go(across(1, 0, 1))
    arrived(1, 1, 1)
    go(across(1, 1, 1))
    arrived(2, 0, 1)
    go(across(2, 0, 1))
    build(*pending.pop(0))
    relay_side()
    arrived(2, 1, 1)
    go(across(2, 1, 1))
    arrived(3, 0, 1)
    go(across(3, 0, 1))
    arrived(3, 1, 1)
    go(across(3, 1, 1))
    build(*pending.pop(0))
    for part in range(2):
        echo_in(1, 0, 1, part)
        pass_echo(6, (1, 0, 1), (1, 1, 1), (0, 0, 1, 0), part)
    while pending:
        build(*pending.pop(0))
    for da in range(2):
        for dc in range(2):
            for part in range(2):
                echo_in(da, 1, dc, part)
    multiply(0, 0, True)
    for turn in range(1, depth):
        multiply(turn, 0, False)
    for turn in range(depth):
        for dk in range(2):
            for dc in range(2):
                crossed(turn, dk, dc)
        multiply(turn, 1, False)

    value = acc[...].reshape(4, 2, feats // 2, 2 * LANES)
    for q in range(4):
        real = value[q, 0, :, :LANES] - value[q, 1, :, LANES:]
        imag = value[q, 0, :, LANES:] + value[q, 1, :, :LANES]
        turned = jnp.concatenate([real, imag], axis=0).T.astype(LOW)
        sbuf[:, q] = turned.reshape(group, own, feats)
    mine = zp * 2 + x
    spread = [(dzp, dx) for dzp in range(depth // 2 - 1, -1, -1) for dx in (1, 0)]
    for dzp, dx in spread:
        slot = dzp * 2 + dx
        if slot:
            to = flip(zp, dzp) * 2 + flip(x, dx)
            go(remote(sbuf.at[to], img0.at[mine], sb_s.at[slot], sb_r.at[slot], device(2 * dzp, dx, 0, 0)))
    img0[mine] = sbuf[mine]
    while len(sent) > group - 1:
        sent.pop(0).wait_send()
    for dzp, dx in spread:
        slot = dzp * 2 + dx
        if slot:
            origin = flip(zp, dzp) * 2 + flip(x, dx)
            remote(
                sbuf.at[origin], img0.at[origin], sb_s.at[slot], sb_r.at[slot], device(2 * dzp, dx, 0, 0)
            ).wait_recv()

    place = (depth // 2, 2, 2, 2)
    wide = 2 * angles

    def child_rows(ref, axis, child, cols):
        split = (place[0] // 2, 2) + place[1:] if axis == 0 else place
        at = 1 if axis == 0 else axis
        whole = ref[...].reshape(split + (own, cols))
        return lax.index_in_dim(whole, child, at, keepdims=False).reshape(-1, cols)

    axis_of = [3, 1, 2] + [0] * (levels - 3)
    pair = jnp.concatenate([child_rows(img0, 3, child, feats) for child in range(2)], axis=1)
    source, target = img_a, img_b
    for side in range(2):
        cols = slice(side * wide, (side + 1) * wide)
        out = low_dot(pair, fold_hi[:, cols]) + low_dot(pair, fold_lo[:, cols])
        source[:, :, :, side] = out.astype(LOW).reshape(place[:3] + (own, wide))
    for level in range(1, levels - 1):
        first, second = (child_rows(source, axis_of[level], child, wide) for child in range(2))
        for side in range(2):
            cols = slice(side * wide, (side + 1) * wide)
            out = low_dot(first, ops[level - 1, 0, :, cols]) + low_dot(second, ops[level - 1, 1, :, cols])
            out = out.astype(LOW)
            if axis_of[level] == 1:
                target[:, side] = out.reshape(place[0], 2, 2, own, wide)
            else:
                target[:, :, side] = out.reshape(place[0], 2, 2, own, wide)
        source, target = target, source
    first, second = (child_rows(source, 0, child, wide) for child in range(2))
    base = HALO + (q_me * group + mine) * own
    block_at = pl.multiple_of(base, HALO)

    for turn in (1, 0):
        side = flip(zp, turn) % 2
        cols = pl.ds(pl.multiple_of(side * wide, wide), wide)
        out = low_dot(first, ops[levels - 2, 0, :, cols]) + low_dot(second, ops[levels - 2, 1, :, cols])
        power = out[:, :angles] * out[:, :angles] + out[:, angles:] * out[:, angles:]
        power = power.astype(LOW).reshape(place[0] // 2, 2, 2, 2, own, angles)
        for pair_at in range(place[0] // 2):
            pbuf[pair_at * 2 + side] = power[pair_at]
        for high in range(place[0] // 2):
            dzp = high * 2 + turn
            for rel in (0, 4, 1, 5, 2, 6, 3, 7):
                dx, dzz, dk = rel // 4, (rel // 2) % 2, rel % 2
                slot = dzp * 8 + rel
                src = pbuf.at[flip(zp, dzp), flip(x, dx), flip(par, dzz), flip(k, dk)]
                if slot:
                    go(
                        remote(
                            src,
                            rows_c.at[pl.ds(block_at, own), :],
                            sc_s.at[slot],
                            sc_r.at[slot],
                            device(2 * dzp + dzz, dx, dk, 0),
                        )
                    )

    rows_c[pl.ds(block_at, own), :] = pbuf[zp, x, par, k]

    @pl.when(c == 0)
    def _():
        rows_c[pl.ds(0, HALO), :] = jnp.zeros((HALO, angles), LOW)

    @pl.when(c == 1)
    def _():
        rows_c[pl.ds(HALO + half, HALO), :] = jnp.zeros((HALO, angles), LOW)

    def landed(slot):
        dzp, rel = slot // 8, slot % 8
        at_zp, at_x = across_bit(zp, dzp), across_bit(x, rel // 4)
        at_par, at_k = across_bit(par, (rel // 2) % 2), across_bit(k, rel % 2)
        at = HALO + ((at_par * 2 + at_k) * group + at_zp * 2 + at_x) * own
        dst = rows_c.at[pl.ds(pl.multiple_of(at, HALO), own), :]
        remote(dst, dst, sc_s.at[slot], sc_r.at[slot], device(0, 0, 0, 1)).wait_recv()

    def across_bit(bit, change):
        return bit + change - 2 * bit * change

    here = ((zp * 2 + x) * 2 + par) * 2 + k
    edge = here * c + (subs - 1 - here) * (1 - c)

    @pl.when(edge != 0)
    def _():
        landed(edge)

    border = remote(
        rows_c.at[pl.ds(pl.multiple_of(half * (1 - c) + HALO * c, HALO), HALO), :],
        rows_c.at[pl.ds(pl.multiple_of((HALO + half) * c, HALO), HALO), :],
        h_s,
        h_r,
        device(0, 0, 0, 1),
    )
    border.start()
    for slot in range(subs - 1, 0, -1):

        @pl.when(edge != slot)
        def _():
            landed(slot)

    far_border = rows_c.at[pl.ds(pl.multiple_of((HALO + half) * (1 - c), HALO), HALO), :]
    remote(far_border, far_border, h_s, h_r, device(0, 0, 0, 1)).wait_recv()
    border.wait_send()
    for copy in sent:
        copy.wait_send()


def smooth_body(chans, power_ref, rate_ref, out_hbm, turned, sem):
    at = lax.axis_index("chan")
    height = turned.shape[1]
    shape = (height + 2 * HALO, LANES)
    row = lax.broadcasted_iota(jnp.int32, shape, 0)
    inside = jnp.logical_and(
        jnp.logical_or(row >= HALO, at > 0), jnp.logical_or(row < HALO + height, at < chans - 1)
    )
    copies = []
    for part in range(turned.shape[0] // LANES):
        cols = slice(part * LANES, (part + 1) * LANES)
        power = power_ref[:, cols].astype(jnp.float32)
        rate = rate_ref[:, cols]
        for sweep in range(PASSES):
            before = pltpu.roll(power, 1, 0)
            after = pltpu.roll(power, shape[0] - 1, 0)
            power = power + rate * (before - 2.0 * power + after)
            power = jnp.where(inside, power, 0.0)
        turned[cols, :] = power[HALO : HALO + height].T
        copy = pltpu.make_async_copy(turned.at[cols, :], out_hbm.at[cols, :], sem.at[part])
        copy.start()
        copies.append(copy)
    for copy in copies:
        copy.wait()


def local_kernel(
    raw_pulses, range_filter, channel_mix, steer_angles, band_offsets, band_weights, smoothing
):
    _, pulses, _, samples = raw_pulses.shape
    _, rows, bins = range_filter.shape
    angles = steer_angles.shape[0]
    levels, _, _, merged, band_width = band_weights.shape
    subs, chans = lax.axis_size("sub"), lax.axis_size("chan")
    half = bins // chans
    group = subs // 4
    own = LANES // group
    depth = subs // 4
    feats = 2 * chans * pulses
    place = (depth // 2, 2, 2, 2)
    dma = pltpu.SemaphoreType.DMA
    vmem = pl.BlockSpec(memory_space=pltpu.VMEM)
    anywhere = pl.BlockSpec(memory_space=pl.ANY)
    power = pl.pallas_call(
        functools.partial(window_body, subs),
        out_shape=jax.ShapeDtypeStruct((half + 2 * HALO, angles), LOW),
        in_specs=[pl.BlockSpec(memory_space=pltpu.HBM)] * 6,
        out_specs=vmem,
        scratch_shapes=[
            pltpu.VMEM((2, chans, chans, pulses), jnp.float32),
            pltpu.VMEM((1, angles), jnp.float32),
            pltpu.VMEM((levels, merged), jnp.int32),
            pltpu.VMEM((levels, 2, 2, band_width, merged), jnp.float32),
            pltpu.VMEM((2, rows, bins), LOW),
            pltpu.VMEM((2, rows, half), LOW),
            pltpu.VMEM((2, subs * chans * rows, LANES), LOW),
            pltpu.VMEM((4, 2, chans, pulses, samples), LOW),
            pltpu.VMEM((4 * feats, 2 * LANES), jnp.float32),
            pltpu.VMEM((2, 2 * angles, 2 * merged), LOW),
            pltpu.VMEM((2, 2 * angles, 2 * merged), LOW),
            pltpu.VMEM((2 * feats, 2 * merged), LOW),
            pltpu.VMEM((2 * feats, 2 * merged), LOW),
            pltpu.VMEM((levels - 1, 2, 2 * angles, 2 * merged), LOW),
            pltpu.VMEM((group, 4, own, feats), LOW),
            pltpu.VMEM((group, 4, own, feats), LOW),
            pltpu.VMEM(place + (own, 2 * angles), LOW),
            pltpu.VMEM(place + (own, 2 * angles), LOW),
            pltpu.VMEM(place + (own, angles), LOW),
            dma((6,)),
            dma,
            dma,
            dma((depth, 2, 2)),
            dma((depth, 2, 2)),
            dma((depth, 2, 2)),
            dma((depth, 2, 2)),
            dma((7, 2)),
            dma((2, 2, 2, 2)),
            dma((group,)),
            dma((group,)),
            dma((subs,)),
            dma((subs,)),
            dma,
            dma,
            pltpu.SemaphoreType.REGULAR((depth - 2,)),
            pltpu.SemaphoreType.REGULAR((depth - 2,)),
        ],
        compiler_params=pltpu.CompilerParams(
            collective_id=0, has_side_effects=True, vmem_limit_bytes=32 << 20
        ),
    )(
        *(
            pltpu.with_memory_space_constraint(array, pltpu.HBM)
            for array in (
                range_filter,
                raw_pulses[:, :, 0, :],
                channel_mix.transpose(0, 2, 3, 1),
                steer_angles[None, :],
                band_offsets,
                band_weights.transpose(0, 1, 2, 4, 3),
            )
        )
    )
    return pl.pallas_call(
        functools.partial(smooth_body, chans),
        out_shape=jax.ShapeDtypeStruct((angles, half), jnp.float32),
        in_specs=[vmem, vmem],
        out_specs=anywhere,
        scratch_shapes=[pltpu.VMEM((angles, half), jnp.float32), dma((angles // LANES,))],
        compiler_params=pltpu.CompilerParams(vmem_limit_bytes=8 << 20),
    )(power, smoothing[None, :])


def fits(mesh, raw_pulses, range_filter, steer_angles, band_offsets):
    subs, chans = mesh.shape["sub"], mesh.shape["chan"]
    rows = range_filter.shape[1] // (subs * chans)
    pulses = raw_pulses.shape[1] // subs
    cut = chans == 2 and subs // 4 == 4
    cut = cut and range_filter.shape[2] == 4 * chans * LANES and LANES // (subs // 4) >= HALO
    cut = cut and rows % 16 == 0 and pulses % 16 == 0 and steer_angles.shape[0] % LANES == 0
    return cut and band_offsets.shape[0] == 4


def solution(mesh):
    in_specs = (
        P(None, "sub", "chan", None),
        P(None, ("sub", "chan"), None),
        P(),
        P(),
        P(),
        P(),
        P("sub"),
    )
    out_specs = P("sub", "chan")

    def run(raw_pulses, range_filter, channel_mix, steer_angles, band_offsets, band_weights, smoothing):
        one = local_kernel if fits(mesh, raw_pulses, range_filter, steer_angles, band_offsets) else local_plain
        part = jax.shard_map(one, mesh=mesh, in_specs=in_specs, out_specs=out_specs, check_vma=False)
        return part(
            raw_pulses, range_filter, channel_mix, steer_angles, band_offsets, band_weights, smoothing
        )

    return run
```
